32 devices in a mesh: gx: 4 (over z), gy: 8 (over y, x, core).
Axes of the slice: x: 2, y: 2, z: 4, core: 2. Of those that a mesh axis runs over, the one named last changes fastest.
Arguments:
- radiance: bfloat16 [2048, 16, 128], P(('gx', 'gy')), may hold values from 0.049804688 to 2
- emission: float32 [2048, 16, 128], P(('gx', 'gy')), may hold values from 0.01 to 1
- reflectance: float32 [2048, 16, 128], P(('gx', 'gy')), may hold values from 0.1 to 0.9
- patch_area: float32 [2048, 128], P(('gx', 'gy')), may hold values from 0.25 to 4
- form_factor: bfloat16 [4096, 128, 128], P(('gx', 'gy')), may hold values from 0.00049972534 to 0.014953613
- source_index: int32 [32, 128], P(('gx', 'gy')), may hold values from 0 to 63
- target_index: int32 [32, 128], P(('gx', 'gy')), may hold values from 0 to 63
- block_index: int32 [32, 128], P(('gx', 'gy')), may hold values from 0 to 127, each once within a row
- valid_count: int32 [32, 32], P(('gx', 'gy')), may hold values from 0 to 4, as said below
Outputs:
- new_radiance: float32 [2048, 16, 128], P(('gx', 'gy'))
The draws below stay inside these ranges and needn't reach their ends.
Inputs may be any that keep to these rules, and one draw needn't show every extreme that they name: `valid_count`: entry [d, p] is the number of live slots among the 4 slots of device d toward peer p, the live ones first; every row has an entry equal to 4. `block_index`: each row is a permutation of 0 to 127.
All inputs are finite; a program needn't handle non-finite values.
Results may differ from the reference program's by a relative error of at most 0.0012.
Values may be sent and summed in bfloat16 or wider, within the bound.
A program may use at most 128 MiB of HBM per device.

```python
import math
import jax
import jax.numpy as jnp
from jax import lax

PATCH = 128
BANDS = 16
CL_DEV = 64
SLOTS = 4
CLUSTERS = 2048
LINKS = 128
DEVICES = 32


def draw_valid_count(key, part):
    base_key = jax.random.fold_in(key, 7)
    heavy_key, count_key, full_key = jax.random.split(base_key, 3)
    heavy_flag = jax.random.randint(heavy_key, (DEVICES, 1), 0, 4) == 0
    lowest = jnp.where(heavy_flag, SLOTS // 2, 0)
    highest = jnp.where(heavy_flag, SLOTS, SLOTS // 2)
    raw_bits = jax.random.randint(count_key, (DEVICES, DEVICES), 0, 1 << 20)
    counts = lowest + raw_bits % (highest - lowest + 1)
    full_peer = jax.random.randint(full_key, (DEVICES,), 0, DEVICES)
    columns = jnp.arange(DEVICES, dtype=jnp.int32)
    counts = jnp.where(columns[None, :] == full_peer[:, None], SLOTS, counts)
    return counts.astype(jnp.int32)


def place_ends(array, rng, smallest, top_value):
    spot = [jax.random.randint(jax.random.fold_in(rng, axis), (), 0, length) for axis, length in enumerate(array.shape)]
    main_axis = array.shape.index(max(array.shape))
    next_to = spot[:main_axis] + [(spot[main_axis] + 1) % array.shape[main_axis]] + spot[main_axis + 1:]
    return array.at[tuple(spot)].set(smallest).at[tuple(next_to)].set(top_value)


def levels(own_key, shape, cuts, low, top_value):
    loudness = 1.0
    for axis_at, shards_of in cuts:
        steps = jax.random.uniform(jax.random.fold_in(jax.random.fold_in(own_key, 6), axis_at), (shards_of,), jnp.float32, low / len(cuts), top_value / len(cuts))
        loudness = loudness * jnp.repeat(jnp.exp(steps), shape[axis_at] // shards_of).reshape((-1,) + (1,) * (len(shape) - 1 - axis_at))
    return loudness


def setup_inputs(seed: int = 0) -> dict:
    seeds = jax.random.split(jax.random.key(seed), 10)
    return {
        "radiance": jnp.clip(jnp.exp(math.log(2.0) - 3.6927934 * jax.random.uniform(seeds[0], (CLUSTERS, BANDS, PATCH), jnp.float32) ** levels(seeds[0], (CLUSTERS, BANDS, PATCH), ((0, 32),), -0.2, 0.2)), 0.049804688, 2.0).astype(jnp.bfloat16),
        "emission": jnp.clip(jnp.exp(math.log(1.0) - 4.6051702 * jax.random.uniform(seeds[1], (CLUSTERS, BANDS, PATCH), jnp.float32) ** levels(seeds[1], (CLUSTERS, BANDS, PATCH), ((0, 32),), -0.2, 0.2)), 0.01, 1.0),
        "reflectance": jnp.clip(jnp.exp(math.log(0.9) - 2.1972245 * jax.random.uniform(seeds[2], (CLUSTERS, BANDS, PATCH), jnp.float32) ** levels(seeds[2], (CLUSTERS, BANDS, PATCH), ((0, 32),), -0.2, 0.2)), 0.1, 0.9),
        "patch_area": jnp.clip(jnp.exp(math.log(4.0) - 2.7725887 * jax.random.uniform(seeds[3], (CLUSTERS, PATCH), jnp.float32) ** levels(seeds[3], (CLUSTERS, PATCH), ((0, 32),), -0.2, 0.2)), 0.25, 4.0),
        "form_factor": jnp.clip(jnp.exp(math.log(0.014953613) - 3.3986496 * jax.random.uniform(seeds[4], (DEVICES * LINKS, PATCH, PATCH), jnp.float32) ** levels(seeds[4], (DEVICES * LINKS, PATCH, PATCH), ((0, 32),), -0.2, 0.2)), 0.00049972534, 0.014953613).astype(jnp.bfloat16),
        "source_index": place_ends(jax.random.randint(seeds[5], (DEVICES, LINKS), 0, CL_DEV), jax.random.fold_in(seeds[5], 1), 0, CL_DEV - 1).astype(jnp.int32),
        "target_index": place_ends(jax.random.randint(seeds[6], (DEVICES, LINKS), 0, CL_DEV), jax.random.fold_in(seeds[6], 1), 0, CL_DEV - 1).astype(jnp.int32),
        "block_index": jax.vmap(lambda own: jax.random.permutation(own, LINKS))(jax.random.split(seeds[7], DEVICES)).reshape((DEVICES, LINKS)).astype(jnp.int32),
        "valid_count": draw_valid_count(jax.random.fold_in(seeds[9], 71), 0),
    }


def reference(radiance, emission, reflectance, patch_area, form_factor, source_index, target_index, block_index, valid_count):
    rad_full = radiance.astype(jnp.float32)
    weighted = (patch_area[:, None, :] * rad_full).astype(jnp.bfloat16)
    weighted_full = weighted.astype(jnp.float32)
    blocks = form_factor.reshape(DEVICES, LINKS, PATCH, PATCH)
    device_ids = jnp.arange(DEVICES, dtype=jnp.int32)

    def step_device(carry, inputs):
        gathered, returned = carry
        device, block_row, source_row, target_row, stored_blocks, live_count = inputs
        position = jnp.arange(LINKS, dtype=jnp.int32)
        peer_ids = (position // SLOTS).astype(jnp.int32)
        live_mask = ((position % SLOTS) < live_count[peer_ids]).astype(jnp.float32)
        source_cluster = (peer_ids * CL_DEV + source_row).astype(jnp.int32)
        target_cluster = (device * CL_DEV + target_row).astype(jnp.int32)
        chosen = stored_blocks[block_row].astype(jnp.float32)
        forward = jnp.einsum("lij,lbj->lbi", chosen, rad_full[source_cluster]) * live_mask[:, None, None]
        backward = jnp.einsum("lij,lbi->lbj", chosen, weighted_full[target_cluster]).astype(jnp.bfloat16)
        backward = lax.optimization_barrier(backward)
        backward = backward.astype(jnp.float32) * live_mask[:, None, None]
        gathered = gathered.at[target_cluster].add(forward)
        returned = returned.at[source_cluster].add(backward)
        return (gathered, returned), None

    zeros_sum = jnp.zeros((CLUSTERS, BANDS, PATCH), jnp.float32)
    (gathered, returned), _ = lax.scan(step_device, (zeros_sum, zeros_sum),
                                       (device_ids, block_index, source_index, target_index, blocks, valid_count))
    irradiance = gathered + returned / patch_area[:, None, :]
    return emission + reflectance * irradiance
```

```python
import functools

import jax
import jax.numpy as jnp
from jax import lax
from jax.experimental import pallas as pl
from jax.experimental.pallas import tpu as pltpu
from jax.sharding import PartitionSpec as P

MESH = pl.DeviceIdType.MESH
GROUP = 4
EXCHANGE_MIB = 60
COMBINE_MIB = 60
F32 = jnp.float32
BF16 = jnp.bfloat16


def exchange(
    outer,
    inner,
    block_hbm,
    target_hbm,
    count_hbm,
    source_hbm,
    rad_hbm,
    area_hbm,
    form_hbm,
    fwd_hbm,
    arrived_hbm,
    asked_hbm,
    block_ref,
    target_ref,
    count_ref,
    source_ref,
    rad_ref,
    area_ref,
    form_ref,
    mirrored_ref,
    weighted_ref,
    bwd_ref,
    served_ref,
    fetched_ref,
    fwd_ref,
    asked_vmem,
    asked_ref,
    form_sem,
    in_sem,
    out_sem,
    send_sems,
    ready_sem,
    mirror_sem,
    idx_sem,
    bwd_sem,
    rad_sem,
):
    n = outer * inner
    half = n // 2
    gx, gy = lax.axis_index("gx"), lax.axis_index("gy")
    me = gx * inner + gy
    mine = me % half
    near = me // half * half
    far = half - near
    mirror = (outer - 1 - gx) * inner + gy
    links = block_ref.shape[1]
    slots = links // n
    clusters = rad_ref.shape[0]
    parts = form_sem.shape[0]
    step = links // parts

    def coords(p):
        return (p // inner, p % inner)

    def mirror_of(p):
        return (outer - 1 - p // inner) * inner + p % inner

    def peer(k):
        return jnp.where(k < half, near, far) + (mine + k) % half

    def origin(k):
        return jnp.where(k < half, near, far) + (mine + n - k) % half

    loads = [
        pltpu.make_async_copy(src, dst, in_sem.at[i])
        for i, (src, dst) in enumerate(
            (
                (rad_hbm, rad_ref),
                (source_hbm, source_ref),
                (area_hbm, area_ref),
                (block_hbm, block_ref),
                (target_hbm, target_ref),
                (count_hbm, count_ref),
            )
        )
    ]
    forms = [
        pltpu.make_async_copy(
            form_hbm.at[pl.ds(i * step, step)], form_ref.at[pl.ds(i * step, step)], form_sem.at[i]
        )
        for i in range(parts)
    ]
    for load in loads + forms:
        load.start()

    barrier = pltpu.get_barrier_semaphore()
    pl.semaphore_signal(barrier, inc=1, device_id=coords(mirror), device_id_type=MESH)

    def greet(k, c):
        pl.semaphore_signal(barrier, inc=1, device_id=coords(peer(k)), device_id_type=MESH)
        return c

    lax.fori_loop(1, half, greet, 0)

    def idx_copy(k):
        return pltpu.make_async_remote_copy(
            src_ref=source_ref,
            dst_ref=asked_vmem.at[me],
            send_sem=send_sems.at[0],
            recv_sem=idx_sem.at[k],
            device_id=coords(peer(k)),
            device_id_type=MESH,
        )

    def bwd_copy(k):
        return pltpu.make_async_remote_copy(
            src_ref=bwd_ref.at[pl.ds(peer(k) * slots, slots)],
            dst_ref=arrived_hbm.at[pl.ds(me * slots, slots)],
            send_sem=send_sems.at[1],
            recv_sem=bwd_sem.at[k],
            device_id=coords(peer(k)),
            device_id_type=MESH,
        )

    def rad_copy(k):
        owner = jnp.where(k < half, me, mirror)
        return pltpu.make_async_remote_copy(
            src_ref=served_ref.at[pl.ds(k * slots, slots)],
            dst_ref=fetched_ref.at[pl.ds(owner * slots, slots)],
            send_sem=send_sems.at[2],
            recv_sem=rad_sem.at[k],
            device_id=coords(near + (mine + k) % half),
            device_id_type=MESH,
        )

    across = pltpu.make_async_remote_copy(
        src_ref=rad_ref,
        dst_ref=mirrored_ref,
        send_sem=mirror_sem.at[0],
        recv_sem=mirror_sem.at[1],
        device_id=coords(mirror),
        device_id_type=MESH,
    )

    for load in loads[:2]:
        load.wait()
    pl.semaphore_wait(barrier, half)
    across.start()
    pl.semaphore_signal(ready_sem, inc=1, device_id=coords(mirror), device_id_type=MESH)

    def send_idx(k, c):
        idx_copy(k).start()
        return c

    lax.fori_loop(1, half, send_idx, 0)
    asked_vmem[me] = source_ref[...]

    for load in loads[2:]:
        load.wait()

    def weigh(c, carry):
        area = area_ref[pl.ds(c, 1), :]
        weighted_ref[c] = (area * rad_ref[c].astype(F32)).astype(BF16)
        return carry

    lax.fori_loop(0, clusters, weigh, 0, unroll=8)

    def live_of(p, s):
        return jnp.where(s < count_ref[0, p], 1.0, 0.0).astype(F32)

    for form in forms:
        form.wait()

    def back(t):
        for u in range(GROUP):
            p = peer(t * GROUP + u)
            for s in range(slots):
                l = p * slots + s
                form = form_ref[block_ref[0, l]]
                seen = weighted_ref[target_ref[0, l]]
                got = jnp.dot(seen, form, preferred_element_type=F32)
                bwd_ref[l] = (got * live_of(p, s)).astype(BF16)

    def back_send(t, c):
        back(t)
        for u in range(GROUP):
            k = t * GROUP + u

            @pl.when(k != 0)
            def _():
                bwd_copy(k).start()

        return c

    def serve(k, c, table_ref, owner):
        p = near + (mine + k) % half
        for s in range(slots):
            served_ref[k * slots + s] = table_ref[asked_ref[p, 0, owner * slots + s]]

        @pl.when(k % half != 0)
        def _():
            rad_copy(k).start()

        return c

    groups = half // GROUP
    lax.fori_loop(0, groups, back_send, 0)
    own = pl.ds(me * slots, slots)
    keep_own = pltpu.make_async_copy(bwd_ref.at[own], arrived_hbm.at[own], out_sem.at[0])
    keep_own.start()

    pl.semaphore_wait(ready_sem, 1)
    lax.fori_loop(half, n, send_idx, 0)
    lax.fori_loop(groups, 2 * groups, back_send, 0)

    def wait_idx(k, c):
        idx_copy(k).wait_recv()
        return c

    lax.fori_loop(1, half, wait_idx, 0)
    side = pl.ds(near, half)
    to_smem = pltpu.make_async_copy(asked_vmem.at[side], asked_ref.at[side], out_sem.at[1])
    to_smem.start()
    to_smem.wait()
    lax.fori_loop(0, half, functools.partial(serve, table_ref=rad_ref, owner=me), 0)
    for s in range(slots):
        fetched_ref[me * slots + s] = served_ref[s]

    def fwd_copy(k, host):
        p = near + (mine + half - k) % half
        rows = pl.ds(jnp.where(host, p, mirror_of(p)) * slots, slots)
        return pltpu.make_async_copy(fwd_ref.at[rows], fwd_hbm.at[rows], out_sem.at[2])

    def forward(t, c, host):
        base = 0 if host else half
        for u in range(GROUP):
            k = t * GROUP + u

            @pl.when(k != 0)
            def _():
                rad_copy(base + k).wait_recv()

        for u in range(GROUP):
            k = t * GROUP + u
            p = near + (mine + half - k) % half
            if not host:
                p = mirror_of(p)
            for s in range(slots):
                l = p * slots + s
                form = form_ref[block_ref[0, l]]
                got = lax.dot_general(
                    fetched_ref[l], form, (((1,), (1,)), ((), ())), preferred_element_type=F32
                )
                fwd_ref[l] = got * live_of(p, s)
        for u in range(GROUP):
            fwd_copy(t * GROUP + u, host).start()
        return c

    across.wait_recv()
    lax.fori_loop(half, n, functools.partial(serve, table_ref=mirrored_ref, owner=mirror), 0)
    for s in range(slots):
        fetched_ref[mirror * slots + s] = served_ref[half * slots + s]

    lax.fori_loop(0, groups, functools.partial(forward, host=True), 0)
    lax.fori_loop(0, groups, functools.partial(forward, host=False), 0)

    lax.fori_loop(half, n, wait_idx, 0)
    keep_asked = pltpu.make_async_copy(asked_vmem, asked_hbm, out_sem.at[1])
    keep_asked.start()

    def wait_bwd(k, c):
        bwd_copy(k).wait_recv()
        return c

    lax.fori_loop(1, n, wait_bwd, 0)
    most = pl.ds(0, (n - 1) * slots)
    pltpu.make_async_copy(bwd_ref.at[most], bwd_ref.at[most], send_sems.at[1]).wait()
    most = pl.ds(0, (n - 2) * slots)
    pltpu.make_async_copy(served_ref.at[most], served_ref.at[most], send_sems.at[2]).wait()
    rows = asked_vmem.at[pl.ds(0, n - 1)]
    pltpu.make_async_copy(rows, rows, send_sems.at[0]).wait()
    across.wait_send()
    keep_own.wait()
    keep_asked.wait()
    pltpu.make_async_copy(fwd_ref, fwd_hbm, out_sem.at[2]).wait()


def combine(
    n,
    inner,
    target_hbm,
    asked_hbm,
    fwd_hbm,
    arrived_hbm,
    em_hbm,
    refl_hbm,
    area_hbm,
    out_hbm,
    em_ref,
    refl_ref,
    area_ref,
    target_ref,
    asked_ref,
    fwd_ref,
    arrived_ref,
    gath,
    ret,
    out_ref,
    in_sem,
    out_sem,
):
    me = lax.axis_index("gx") * inner + lax.axis_index("gy")
    clusters = em_ref.shape[0]
    links = fwd_ref.shape[0]
    slots = links // n
    base = me * slots
    parts = out_sem.shape[0]
    step = clusters // parts
    loads = [
        pltpu.make_async_copy(src, dst, in_sem.at[i])
        for i, (src, dst) in enumerate(
            (
                (fwd_hbm, fwd_ref),
                (arrived_hbm, arrived_ref),
                (target_hbm, target_ref),
                (asked_hbm, asked_ref),
                (em_hbm, em_ref),
                (refl_hbm, refl_ref),
                (area_hbm, area_ref),
            )
        )
    ]
    for load in loads:
        load.start()

    def clear(c, carry):
        gath[c] = jnp.zeros(gath.shape[1:], F32)
        ret[c] = jnp.zeros(ret.shape[1:], F32)
        return carry

    lax.fori_loop(0, clusters, clear, 0, unroll=8)
    for load in loads[:4]:
        load.wait()

    def scatter(p, carry):
        for s in range(slots):
            l = p * slots + s
            t = target_ref[0, l]
            c = asked_ref[p, 0, base + s]
            gath[t] += fwd_ref[l]
            ret[c] += arrived_ref[l].astype(F32)
        return carry

    lax.fori_loop(0, n, scatter, 0, unroll=2)

    def finish(c, carry):
        area = area_ref[pl.ds(c, 1), :]
        out_ref[c] = em_ref[c] + refl_ref[c] * (gath[c] + ret[c] / area)
        return carry

    for load in loads[4:]:
        load.wait()
    stores = []
    for i in range(parts):
        lax.fori_loop(i * step, (i + 1) * step, finish, 0, unroll=8)
        rows = pl.ds(i * step, step)
        stores.append(pltpu.make_async_copy(out_ref.at[rows], out_hbm.at[rows], out_sem.at[i]))
        stores[-1].start()
    for store in stores:
        store.wait()


def solution(mesh):
    outer, inner = mesh.shape["gx"], mesh.shape["gy"]
    n = outer * inner

    def shards(
        radiance,
        emission,
        reflectance,
        patch_area,
        form_factor,
        source_index,
        target_index,
        block_index,
        valid_count,
    ):
        clusters, bands, patches = radiance.shape
        links = source_index.shape[1]
        slots = links // n
        tile = (bands, patches)
        hbm = pl.BlockSpec(memory_space=pl.ANY)
        parts = 4
        fwd, arrived, asked = pl.pallas_call(
            functools.partial(exchange, outer, inner),
            out_shape=(
                jax.ShapeDtypeStruct((links,) + tile, F32),
                jax.ShapeDtypeStruct((links,) + tile, BF16),
                jax.ShapeDtypeStruct((n, 1, links), jnp.int32),
            ),
            in_specs=[hbm] * 7,
            out_specs=(hbm, hbm, hbm),
            scratch_shapes=[
                pltpu.SMEM(block_index.shape, jnp.int32),
                pltpu.SMEM(target_index.shape, jnp.int32),
                pltpu.SMEM(valid_count.shape, jnp.int32),
                pltpu.VMEM(source_index.shape, jnp.int32),
                pltpu.VMEM(radiance.shape, BF16),
                pltpu.VMEM(patch_area.shape, F32),
                pltpu.VMEM(form_factor.shape, BF16),
                pltpu.VMEM((clusters,) + tile, BF16),
                pltpu.VMEM((clusters,) + tile, BF16),
                pltpu.VMEM((links,) + tile, BF16),
                pltpu.VMEM((links,) + tile, BF16),
                pltpu.VMEM((links,) + tile, BF16),
                pltpu.VMEM((links,) + tile, F32),
                pltpu.VMEM((n, 1, links), jnp.int32),
                pltpu.SMEM((n, 1, links), jnp.int32),
                pltpu.SemaphoreType.DMA((parts,)),
                pltpu.SemaphoreType.DMA((6,)),
                pltpu.SemaphoreType.DMA((3,)),
                pltpu.SemaphoreType.DMA((3,)),
                pltpu.SemaphoreType.REGULAR,
                pltpu.SemaphoreType.DMA((2,)),
                pltpu.SemaphoreType.DMA((n,)),
                pltpu.SemaphoreType.DMA((n,)),
                pltpu.SemaphoreType.DMA((n,)),
            ],
            compiler_params=pltpu.CompilerParams(
                collective_id=0, has_side_effects=True, vmem_limit_bytes=EXCHANGE_MIB * 1024 * 1024
            ),
            name="exchange",
        )(
            block_index,
            target_index,
            valid_count,
            source_index,
            radiance,
            patch_area,
            form_factor,
        )
        return pl.pallas_call(
            functools.partial(combine, n, inner),
            out_shape=jax.ShapeDtypeStruct((clusters,) + tile, F32),
            in_specs=[hbm] * 7,
            out_specs=hbm,
            scratch_shapes=[
                pltpu.VMEM((clusters,) + tile, F32),
                pltpu.VMEM((clusters,) + tile, F32),
                pltpu.VMEM(patch_area.shape, F32),
                pltpu.SMEM(target_index.shape, jnp.int32),
                pltpu.SMEM((n, 1, links), jnp.int32),
                pltpu.VMEM((links,) + tile, F32),
                pltpu.VMEM((links,) + tile, BF16),
                pltpu.VMEM((clusters,) + tile, F32),
                pltpu.VMEM((clusters,) + tile, F32),
                pltpu.VMEM((clusters,) + tile, F32),
                pltpu.SemaphoreType.DMA((7,)),
                pltpu.SemaphoreType.DMA((4,)),
            ],
            compiler_params=pltpu.CompilerParams(vmem_limit_bytes=COMBINE_MIB * 1024 * 1024),
            name="combine",
        )(target_index, asked, fwd, arrived, emission, reflectance, patch_area)

    spec3 = P(("gx", "gy"), None, None)
    spec2 = P(("gx", "gy"), None)
    return jax.shard_map(
        shards,
        mesh=mesh,
        in_specs=(spec3, spec3, spec3, spec2, spec3, spec2, spec2, spec2, spec2),
        out_specs=spec3,
        check_vma=False,
    )
```

```python
import functools

import jax
import jax.numpy as jnp
from jax import lax
from jax.experimental import pallas as pl
from jax.experimental.pallas import tpu as pltpu
from jax.sharding import PartitionSpec as P

MESH = pl.DeviceIdType.MESH
GROUP = 4
EXCHANGE_MIB = 60
F32 = jnp.float32
BF16 = jnp.bfloat16


def exchange(
    outer,
    inner,
    block_hbm,
    target_hbm,
    count_hbm,
    source_hbm,
    rad_hbm,
    area_hbm,
    form_hbm,
    em_hbm,
    refl_hbm,
    out_ref,
    block_ref,
    target_ref,
    count_ref,
    source_ref,
    rad_ref,
    area_ref,
    form_ref,
    mirrored_ref,
    weighted_ref,
    bwd_ref,
    served_ref,
    fetched_ref,
    arrived_ref,
    gath_ref,
    ret_ref,
    em_ref,
    refl_ref,
    asked_vmem,
    asked_ref,
    keys_ref,
    chain_vmem,
    chain_ref,
    form_sem,
    in_sem,
    out_sem,
    send_sems,
    ready_sem,
    mirror_sem,
    idx_sem,
    bwd_sem,
    rad_sem,
):
    n = outer * inner
    half = n // 2
    gx, gy = lax.axis_index("gx"), lax.axis_index("gy")
    me = gx * inner + gy
    mine = me % half
    near = me // half * half
    far = half - near
    mirror = (outer - 1 - gx) * inner + gy
    links = block_ref.shape[1]
    slots = links // n
    clusters = rad_ref.shape[0]
    lanes = keys_ref.shape[1]
    parts = form_sem.shape[0]
    step = links // parts

    def coords(p):
        return (p // inner, p % inner)

    def mirror_of(p):
        return (outer - 1 - p // inner) * inner + p % inner

    def peer(k):
        return near + (mine + k) % half

    def far_peer(k):
        plane = k // inner
        return jnp.where(near == 0, outer - 1 - plane, plane) * inner + (gy + k) % inner

    loads = [
        pltpu.make_async_copy(src, dst, in_sem.at[i])
        for i, (src, dst) in enumerate(
            (
                (rad_hbm, rad_ref),
                (source_hbm, source_ref),
                (area_hbm, area_ref),
                (block_hbm, block_ref),
                (target_hbm, target_ref),
                (count_hbm, count_ref),
                (em_hbm, em_ref),
                (refl_hbm, refl_ref),
            )
        )
    ]
    forms = [
        pltpu.make_async_copy(
            form_hbm.at[pl.ds(i * step, step)], form_ref.at[pl.ds(i * step, step)], form_sem.at[i]
        )
        for i in range(parts)
    ]
    for load in loads[:6] + forms + loads[6:]:
        load.start()

    barrier = pltpu.get_barrier_semaphore()
    pl.semaphore_signal(barrier, inc=1, device_id=coords(mirror), device_id_type=MESH)

    def greet(k, c):
        pl.semaphore_signal(barrier, inc=1, device_id=coords(peer(k)), device_id_type=MESH)
        return c

    lax.fori_loop(1, half, greet, 0)

    def idx_copy(to, sender=me, src_ref=source_ref):
        return pltpu.make_async_remote_copy(
            src_ref=src_ref,
            dst_ref=asked_vmem.at[sender],
            send_sem=send_sems.at[0],
            recv_sem=idx_sem.at[sender],
            device_id=coords(to),
            device_id_type=MESH,
        )

    def bwd_copy(to, sender=me):
        return pltpu.make_async_remote_copy(
            src_ref=bwd_ref.at[pl.ds(to * slots, slots)],
            dst_ref=arrived_ref.at[pl.ds(sender * slots, slots)],
            send_sem=send_sems.at[1],
            recv_sem=bwd_sem.at[sender],
            device_id=coords(to),
            device_id_type=MESH,
        )

    def rad_copy(to, owner, row):
        return pltpu.make_async_remote_copy(
            src_ref=served_ref.at[pl.ds(row * slots, slots)],
            dst_ref=fetched_ref.at[pl.ds(owner * slots, slots)],
            send_sem=send_sems.at[2],
            recv_sem=rad_sem.at[owner],
            device_id=coords(to),
            device_id_type=MESH,
        )

    share = clusters // mirror_sem.shape[1]
    across = [
        pltpu.make_async_remote_copy(
            src_ref=rad_ref.at[pl.ds(i * share, share)],
            dst_ref=mirrored_ref.at[pl.ds(i * share, share)],
            send_sem=mirror_sem.at[0, i],
            recv_sem=mirror_sem.at[1, i],
            device_id=coords(mirror),
            device_id_type=MESH,
        )
        for i in range(mirror_sem.shape[1])
    ]

    def send_idx(k, c):
        idx_copy(peer(k)).start()
        return c

    def relay_idx(k, c):
        idx_copy(peer(k), mirror, asked_vmem.at[mirror]).start()
        return c

    for load in loads[:2]:
        load.wait()
    pl.semaphore_wait(barrier, half)
    idx_copy(mirror).start()
    lax.fori_loop(1, half, send_idx, 0)
    for copy in across:
        copy.start()
    pl.semaphore_signal(ready_sem, inc=1, device_id=coords(mirror), device_id_type=MESH)
    asked_vmem[me] = source_ref[...]

    for load in loads[2:6]:
        load.wait()

    def weigh(c, carry):
        area = area_ref[pl.ds(c, 1), :]
        weighted_ref[c] = (area * rad_ref[c].astype(F32)).astype(BF16)
        return carry

    lax.fori_loop(0, clusters, weigh, 0, unroll=8)

    def live_of(p, s):
        return jnp.where(s < count_ref[0, p], 1.0, 0.0).astype(F32)

    for form in forms:
        form.wait()

    def back(p):
        for s in range(slots):
            l = p * slots + s
            form = form_ref[block_ref[0, l]]
            seen = weighted_ref[target_ref[0, l]]
            got = jnp.dot(seen, form, preferred_element_type=F32)
            bwd_ref[l] = (got * live_of(p, s)).astype(BF16)

    def back_near(t, c):
        for u in range(GROUP):
            back(peer(t * GROUP + u))
        for u in range(GROUP):
            k = t * GROUP + u

            @pl.when(k != 0)
            def _():
                bwd_copy(peer(k)).start()

        return c

    def back_far(t, c):
        for u in range(GROUP):
            back(far_peer(t * GROUP + u))
        return c

    def send_far(k, c):
        bwd_copy(far_peer(k)).start()
        return c

    def serve(k, c, table_ref, owner, base):
        p = peer(k)
        for s in range(slots):
            served_ref[(base + k) * slots + s] = table_ref[asked_ref[p, 0, owner * slots + s]]

        @pl.when(k != 0)
        def _():
            rad_copy(p, owner, base + k).start()

        return c

    groups = half // GROUP
    lax.fori_loop(0, groups, back_near, 0)
    for s in range(slots):
        arrived_ref[me * slots + s] = bwd_ref[me * slots + s]
    lax.fori_loop(0, groups, back_far, 0)

    def wait_idx(k, c):
        idx_copy(me, peer(k)).wait_recv()
        return c

    def wait_idx_far(k, c):
        idx_copy(me, mirror_of(peer(k))).wait_recv()
        return c

    idx_copy(me, mirror).wait_recv()
    lax.fori_loop(1, half, relay_idx, 0)
    lax.fori_loop(1, half, wait_idx, 0)
    side = pl.ds(near, half)
    to_smem = pltpu.make_async_copy(asked_vmem.at[side], asked_ref.at[side], out_sem.at[2])
    to_smem.start()
    to_smem.wait()
    lax.fori_loop(0, half, functools.partial(serve, table_ref=rad_ref, owner=me, base=0), 0)
    for s in range(slots):
        fetched_ref[me * slots + s] = served_ref[s]

    pl.semaphore_wait(ready_sem, 1)
    for copy in across[:-1]:
        copy.wait_send()
    lax.fori_loop(0, half, send_far, 0)

    def link_chain(near_key, far_key, row):
        def fill(k, c, key, base):
            for s in range(slots):
                keys_ref[pl.ds((base + k) * slots + s, 1), :] = jnp.full((1, lanes), key(k, s), jnp.int32)
            return c

        lax.fori_loop(0, half, functools.partial(fill, key=near_key, base=0), 0, unroll=2)
        lax.fori_loop(0, half, functools.partial(fill, key=far_key, base=half), 0, unroll=2)
        keys = keys_ref[...]
        order = lax.broadcasted_iota(jnp.int32, keys.shape, 0)
        lane = lax.broadcasted_iota(jnp.int32, keys.shape, 1)
        for i in range(links // lanes):
            at = lane + i * lanes
            key = jnp.max(jnp.where(order == at, keys, -1), axis=0, keepdims=True)
            before = jnp.max(
                jnp.where((keys == key) & (order < at), order, -1), axis=0, keepdims=True
            )
            chain_vmem[row, :, pl.ds(i * lanes, lanes)] = jnp.where(before < 0, links, before)
        last = jnp.max(jnp.where(keys == lane, order, -1), axis=0, keepdims=True)
        chain_vmem[row + 1, :, pl.ds(0, lanes)] = jnp.where(last < 0, links, last)
        rows = pl.ds(row, 2)
        return pltpu.make_async_copy(chain_vmem.at[rows], chain_ref.at[rows], out_sem.at[row // 2])

    def summed(ref, row, at):
        return ref[chain_ref[row, 0, at]]

    def target_key(k, s):
        return target_ref[0, peer(k) * slots + s]

    def target_key_far(k, s):
        return target_ref[0, mirror_of(peer(k)) * slots + s]

    def source_key(k, s):
        return asked_ref[peer(k), 0, me * slots + s]

    def source_key_far(k, s):
        return asked_ref[far_peer(k), 0, me * slots + s]

    def forward(t, c, host):
        owners = [peer(t * GROUP + u) for u in range(GROUP)]
        if not host:
            owners = [mirror_of(p) for p in owners]
        for u, p in enumerate(owners):

            @pl.when(t * GROUP + u != 0)
            def _():
                rad_copy(me, p, 0).wait_recv()

        got = []
        for p in owners:
            for s in range(slots):
                l = p * slots + s
                form = form_ref[block_ref[0, l]]
                seen = lax.dot_general(
                    fetched_ref[l], form, (((1,), (1,)), ((), ())), preferred_element_type=F32
                )
                got.append(seen * live_of(p, s))
        first = ((0 if host else half) + t * GROUP) * slots
        for i, term in enumerate(got):
            gath_ref[first + i] = term + summed(gath_ref, 0, first + i)
        return c

    gath_ref[links] = jnp.zeros(gath_ref.shape[1:], F32)
    ret_ref[links] = jnp.zeros(ret_ref.shape[1:], F32)
    by_target = link_chain(target_key, target_key_far, 0)
    by_target.start()
    lax.fori_loop(1, half, wait_idx_far, 0)
    beyond = pl.ds(far, half)
    to_smem = pltpu.make_async_copy(asked_vmem.at[beyond], asked_ref.at[beyond], out_sem.at[2])
    to_smem.start()
    to_smem.wait()
    by_source = link_chain(source_key, source_key_far, 2)
    by_source.start()
    by_target.wait()

    by_source.wait()

    for copy in across:
        copy.wait_recv()
    lax.fori_loop(
        0, half, functools.partial(serve, table_ref=mirrored_ref, owner=mirror, base=half), 0
    )
    for s in range(slots):
        fetched_ref[mirror * slots + s] = served_ref[half * slots + s]

    lax.fori_loop(0, groups, functools.partial(forward, host=True), 0)
    lax.fori_loop(0, groups, functools.partial(forward, host=False), 0)

    def blend(c, carry):
        area = area_ref[pl.ds(c, 1), :]
        em_ref[c] = em_ref[c] + refl_ref[c] * summed(gath_ref, 1, c)
        refl_ref[c] = refl_ref[c] / area
        return carry

    for load in loads[6:]:
        load.wait()
    lax.fori_loop(0, clusters, blend, 0, unroll=8)

    def collect(k, c, peers, base, skip):
        p = peers(k)

        @pl.when(k != skip)
        def _():
            bwd_copy(me, p).wait_recv()

        for s in range(slots):
            i = (base + k) * slots + s
            ret_ref[i] = arrived_ref[p * slots + s].astype(F32) + summed(ret_ref, 2, i)
        return c

    lax.fori_loop(0, half, functools.partial(collect, peers=peer, base=0, skip=0), 0)
    lax.fori_loop(0, half, functools.partial(collect, peers=far_peer, base=half, skip=half), 0)

    def finish(c, carry):
        out_ref[c] = em_ref[c] + refl_ref[c] * summed(ret_ref, 3, c)
        return carry

    lax.fori_loop(0, clusters, finish, 0, unroll=8)
    most = pl.ds(0, (n - 1) * slots)
    pltpu.make_async_copy(bwd_ref.at[most], bwd_ref.at[most], send_sems.at[1]).wait()
    most = pl.ds(0, (n - 2) * slots)
    pltpu.make_async_copy(served_ref.at[most], served_ref.at[most], send_sems.at[2]).wait()
    rows = asked_vmem.at[pl.ds(0, n - 1)]
    pltpu.make_async_copy(rows, rows, send_sems.at[0]).wait()
    across[-1].wait_send()


def solution(mesh):
    outer, inner = mesh.shape["gx"], mesh.shape["gy"]
    n = outer * inner

    def shards(
        radiance,
        emission,
        reflectance,
        patch_area,
        form_factor,
        source_index,
        target_index,
        block_index,
        valid_count,
    ):
        clusters, bands, patches = radiance.shape
        links = source_index.shape[1]
        slots = links // n
        tile = (bands, patches)
        hbm = pl.BlockSpec(memory_space=pl.ANY)
        parts = 4
        return pl.pallas_call(
            functools.partial(exchange, outer, inner),
            out_shape=pltpu.VMEM((clusters,) + tile, F32),
            in_specs=[hbm] * 9,
            out_specs=pl.BlockSpec(memory_space=pltpu.VMEM),
            scratch_shapes=[
                pltpu.SMEM(block_index.shape, jnp.int32),
                pltpu.SMEM(target_index.shape, jnp.int32),
                pltpu.SMEM(valid_count.shape, jnp.int32),
                pltpu.VMEM(source_index.shape, jnp.int32),
                pltpu.VMEM(radiance.shape, BF16),
                pltpu.VMEM(patch_area.shape, F32),
                pltpu.VMEM(form_factor.shape, BF16),
                pltpu.VMEM((clusters,) + tile, BF16),
                pltpu.VMEM((clusters,) + tile, BF16),
                pltpu.VMEM((links,) + tile, BF16),
                pltpu.VMEM((links,) + tile, BF16),
                pltpu.VMEM((links,) + tile, BF16),
                pltpu.VMEM((links,) + tile, BF16),
                pltpu.VMEM((links + 1,) + tile, F32),
                pltpu.VMEM((links + 1,) + tile, F32),
                pltpu.VMEM((clusters,) + tile, F32),
                pltpu.VMEM((clusters,) + tile, F32),
                pltpu.VMEM((n, 1, links), jnp.int32),
                pltpu.SMEM((n, 1, links), jnp.int32),
                pltpu.VMEM((links, patches), jnp.int32),
                pltpu.VMEM((4, 1, links), jnp.int32),
                pltpu.SMEM((4, 1, links), jnp.int32),
                pltpu.SemaphoreType.DMA((parts,)),
                pltpu.SemaphoreType.DMA((8,)),
                pltpu.SemaphoreType.DMA((3,)),
                pltpu.SemaphoreType.DMA((3,)),
                pltpu.SemaphoreType.REGULAR,
                pltpu.SemaphoreType.DMA((2, 4)),
                pltpu.SemaphoreType.DMA((n,)),
                pltpu.SemaphoreType.DMA((n,)),
                pltpu.SemaphoreType.DMA((n,)),
            ],
            compiler_params=pltpu.CompilerParams(
                collective_id=0, has_side_effects=True, vmem_limit_bytes=EXCHANGE_MIB * 1024 * 1024
            ),
            name="exchange",
        )(
            block_index,
            target_index,
            valid_count,
            source_index,
            radiance,
            patch_area,
            form_factor,
            emission,
            reflectance,
        )

    spec3 = P(("gx", "gy"), None, None)
    spec2 = P(("gx", "gy"), None)
    return jax.shard_map(
        shards,
        mesh=mesh,
        in_specs=(spec3, spec3, spec3, spec2, spec3, spec2, spec2, spec2, spec2),
        out_specs=spec3,
        check_vma=False,
    )
```

```python
import functools

import jax
import jax.numpy as jnp
from jax import lax
from jax.experimental import pallas as pl
from jax.experimental.pallas import tpu as pltpu
from jax.sharding import PartitionSpec as P

MESH = pl.DeviceIdType.MESH
GROUP = 4
EXCHANGE_MIB = 60
F32 = jnp.float32
BF16 = jnp.bfloat16


def exchange(
    outer,
    inner,
    block_hbm,
    target_hbm,
    count_hbm,
    source_hbm,
    rad_hbm,
    area_hbm,
    form_hbm,
    em_hbm,
    refl_hbm,
    out_ref,
    block_ref,
    target_ref,
    count_ref,
    source_ref,
    rad_ref,
    area_ref,
    form_ref,
    tables,
    weighted_ref,
    bwd_ref,
    served_ref,
    fetched_ref,
    arrived_ref,
    gath_ref,
    ret_ref,
    em_ref,
    refl_ref,
    part_ref,
    asked_vmem,
    asked_ref,
    keys_ref,
    chain_vmem,
    chain_ref,
    form_sem,
    in_sem,
    out_sem,
    send_sems,
    ready_sem,
    round_sem,
    mirror_sem,
    idx_sem,
    bwd_sem,
    rad_sem,
):
    n = outer * inner
    half = n // 2
    gx, gy = lax.axis_index("gx"), lax.axis_index("gy")
    me = gx * inner + gy
    mine = me % half
    near = me // half * half
    far = half - near
    planes = outer // 2
    depth = jnp.where(near == 0, gx, outer - 1 - gx)
    is_gate = depth == planes - 1
    gate = jnp.where(near == 0, planes, planes - 1) * inner + gy
    links = block_ref.shape[1]
    slots = links // n
    clusters = rad_ref.shape[0]
    lanes = keys_ref.shape[1]
    parts = 4
    step = links // parts
    groups = half // GROUP

    def coords(p):
        return (p // inner, p % inner)

    def peer(k):
        return near + (mine + k) % half

    def far_plane(j):
        return jnp.where(near == 0, outer - 1 - j, j) * inner

    def far_peer(k):
        return far_plane(k // inner) + (gy + k) % inner

    loads = [
        pltpu.make_async_copy(src, dst, in_sem.at[i])
        for i, (src, dst) in enumerate(
            (
                (rad_hbm, rad_ref),
                (source_hbm, source_ref),
                (area_hbm, area_ref),
                (block_hbm, block_ref),
                (target_hbm, target_ref),
                (count_hbm, count_ref),
                (em_hbm, em_ref),
                (refl_hbm, refl_ref),
            )
        )
    ]
    forms = [
        pltpu.make_async_copy(
            form_hbm.at[pl.ds(i * step, step)], form_ref.at[pl.ds(i * step, step)], form_sem
        )
        for i in range(parts)
    ]
    for load in loads[:6] + forms + loads[6:]:
        load.start()

    def beside(j):
        bit = 1 << j
        return near + mine + bit - 2 * bit * (mine // bit % 2)

    barrier = pltpu.get_barrier_semaphore()
    bits = half.bit_length() - 1
    for j in range(bits):
        pl.semaphore_signal(barrier, inc=1, device_id=coords(beside(j)), device_id_type=MESH)

    @pl.when(is_gate)
    def _():
        for j in range(planes):
            pl.semaphore_signal(
                barrier, inc=1, device_id=coords(far_plane(j) + gy), device_id_type=MESH
            )

    def settle(ref, rows, sem):
        part = ref.at[pl.ds(0, rows)]
        pltpu.make_async_copy(part, part, sem).wait()

    def idx_copy(to, which, sender=me, src_ref=source_ref):
        return pltpu.make_async_remote_copy(
            src_ref=src_ref,
            dst_ref=asked_vmem.at[sender],
            send_sem=send_sems.at[0],
            recv_sem=idx_sem.at[which],
            device_id=coords(to),
            device_id_type=MESH,
        )

    def bwd_copy(to, which):
        return pltpu.make_async_remote_copy(
            src_ref=bwd_ref.at[pl.ds(to * slots, slots)],
            dst_ref=arrived_ref.at[pl.ds(me * slots, slots)],
            send_sem=send_sems.at[1],
            recv_sem=bwd_sem.at[which],
            device_id=coords(to),
            device_id_type=MESH,
        )

    def rad_copy(to, owner, row, which):
        return pltpu.make_async_remote_copy(
            src_ref=served_ref.at[pl.ds(row * slots, slots)],
            dst_ref=fetched_ref.at[pl.ds(owner * slots, slots)],
            send_sem=send_sems.at[2],
            recv_sem=rad_sem.at[which],
            device_id=coords(to),
            device_id_type=MESH,
        )

    pieces = 4
    share = clusters // pieces
    def across(i, j):
        part = pl.ds(i * share, share)
        return pltpu.make_async_remote_copy(
            src_ref=rad_ref.at[part],
            dst_ref=tables[j].at[part],
            send_sem=mirror_sem.at[0 if i < pieces - 1 else 1],
            recv_sem=mirror_sem.at[2 + j],
            device_id=coords(gate),
            device_id_type=MESH,
        )

    def send_pieces(first, end):
        for j in range(planes):

            @pl.when(depth == j)
            def _():
                for i in range(first, end):
                    across(i, j).start()

    def send_idx(k, c):
        idx_copy(peer(k), 0).start()
        return c

    def relay_idx(k, c):
        for j in range(planes):
            owner = far_plane(j) + gy
            idx_copy(peer(k), 2, owner, asked_vmem.at[owner]).start()
        return c

    def tell(j):
        pl.semaphore_signal(round_sem.at[j], inc=1, device_id=coords(beside(j)), device_id_type=MESH)

    for load in loads[:2]:
        load.wait()
    pl.semaphore_wait(barrier, bits + 1)
    idx_copy(gate, 1).start()
    send_pieces(0, pieces // 2)
    tell(0)
    asked_vmem[me] = source_ref[...]
    for load in loads[2:6]:
        load.wait()
    for j in range(bits - 1):
        pl.semaphore_wait(round_sem.at[j], 1)
        if j + 1 < bits - 1:
            tell(j + 1)
    lax.fori_loop(1, half, send_idx, 0)

    @pl.when(is_gate)
    def _():
        pl.semaphore_signal(ready_sem, inc=1, device_id=coords(gate), device_id_type=MESH)

    send_pieces(pieces // 2, pieces)

    def weigh(c, carry):
        area = area_ref[pl.ds(c, 1), :]
        weighted_ref[c] = (area * rad_ref[c].astype(F32)).astype(BF16)
        return carry

    lax.fori_loop(0, clusters, weigh, 0, unroll=8)

    def live_of(p, s):
        return jnp.where(s < count_ref[0, p], 1.0, 0.0).astype(F32)

    pltpu.make_async_copy(form_hbm, form_ref, form_sem).wait()

    def back(p):
        for s in range(slots):
            l = p * slots + s
            form = form_ref[block_ref[0, l]]
            seen = weighted_ref[target_ref[0, l]]
            got = jnp.dot(seen, form, preferred_element_type=F32)
            bwd_ref[l] = (got * live_of(p, s)).astype(BF16)

    def back_near(t, c):
        for u in range(GROUP):
            back(peer(t * GROUP + u))
        return c

    def back_far(t, c):
        for u in range(GROUP):
            back(far_peer(t * GROUP + u))
        return c

    def send_near(k, c):
        bwd_copy(peer(k), 0).start()
        return c

    def send_far(k, c):
        at = depth * inner + (inner - k % inner) % inner
        bwd_copy(far_peer(k), 1 + at // GROUP).start()
        return c

    def serve(k, c):
        p = peer(k)
        for s in range(slots):
            served_ref[k * slots + s] = rad_ref[asked_ref[p, 0, me * slots + s]]

        @pl.when(k != 0)
        def _():
            rad_copy(p, me, k, (half - k) % half // GROUP).start()

        return c

    def serve_table(k, c, j):
        p = peer(k)
        owner = far_plane(j) + gy
        base = (1 + j) * half + k
        for s in range(slots):
            served_ref[base * slots + s] = tables[j][asked_ref[p, 0, owner * slots + s]]

        @pl.when(k != 0)
        def _():
            at = j * inner + (inner - k % inner) % inner
            rad_copy(p, owner, base, groups + at // GROUP).start()

        return c

    def open_table(j):
        settle(rad_ref, clusters, mirror_sem.at[2 + j])
        lax.fori_loop(0, half, functools.partial(serve_table, j=j), 0)
        owner = far_plane(j) + gy
        for s in range(slots):
            fetched_ref[owner * slots + s] = served_ref[(1 + j) * half * slots + s]

    lax.fori_loop(0, groups, back_near, 0)
    lax.fori_loop(1, half, send_near, 0)
    for s in range(slots):
        arrived_ref[me * slots + s] = bwd_ref[me * slots + s]
    lax.fori_loop(0, groups, back_far, 0)

    @pl.when(is_gate)
    def _():
        settle(asked_vmem, planes, idx_sem.at[1])
        lax.fori_loop(1, half, relay_idx, 0)

    settle(asked_vmem, half - 1, idx_sem.at[0])
    side = pl.ds(near, half)
    to_smem = pltpu.make_async_copy(asked_vmem.at[side], asked_ref.at[side], out_sem.at[2])
    to_smem.start()
    to_smem.wait()
    lax.fori_loop(0, half, serve, 0)
    for s in range(slots):
        fetched_ref[me * slots + s] = served_ref[s]

    @pl.when(is_gate)
    def _():
        for j in range(planes - 1):
            open_table(j)

    settle(rad_ref, clusters - share, mirror_sem.at[0])
    pl.semaphore_wait(ready_sem, 1)

    @pl.when(is_gate)
    def _():
        for j in range(1, planes):
            p = near + (mine + j * inner) % half
            pl.semaphore_signal(ready_sem, inc=1, device_id=coords(p), device_id_type=MESH)

    lax.fori_loop(0, half, send_far, 0)

    def link_chain(near_key, far_key, row):
        def fill(k, c, key, base):
            for s in range(slots):
                keys_ref[pl.ds((base + k) * slots + s, 1), :] = jnp.full((1, lanes), key(k, s), jnp.int32)
            return c

        lax.fori_loop(0, half, functools.partial(fill, key=near_key, base=0), 0, unroll=2)
        lax.fori_loop(0, half, functools.partial(fill, key=far_key, base=half), 0, unroll=2)
        keys = keys_ref[...]
        order = lax.broadcasted_iota(jnp.int32, keys.shape, 0)
        lane = lax.broadcasted_iota(jnp.int32, keys.shape, 1)
        for i in range(links // lanes):
            at = lane + i * lanes
            key = jnp.max(jnp.where(order == at, keys, -1), axis=0, keepdims=True)
            before = jnp.max(
                jnp.where((keys == key) & (order < at), order, -1), axis=0, keepdims=True
            )
            chain_vmem[row, :, pl.ds(i * lanes, lanes)] = jnp.where(before < 0, links, before)
        last = jnp.max(jnp.where(keys == lane, order, -1), axis=0, keepdims=True)
        chain_vmem[row + 1, :, pl.ds(0, lanes)] = jnp.where(last < 0, links, last)
        rows = pl.ds(row, 2)
        return pltpu.make_async_copy(chain_vmem.at[rows], chain_ref.at[rows], out_sem.at[row // 2])

    def summed(ref, row, at):
        return ref[chain_ref[row, 0, at]]

    def target_key(k, s):
        return target_ref[0, peer(k) * slots + s]

    def target_key_far(k, s):
        return target_ref[0, far_peer(k) * slots + s]

    def source_key(k, s):
        return asked_ref[peer(k), 0, me * slots + s]

    def source_key_far(k, s):
        return asked_ref[far_peer(k), 0, me * slots + s]

    def forward(t, c, host):
        owners = [(peer if host else far_peer)(t * GROUP + u) for u in range(GROUP)]
        here = (t == 0) if host else is_gate & (t * GROUP % inner == 0)
        sem = rad_sem.at[t if host else groups + t]

        @pl.when(here)
        def _():
            settle(fetched_ref, (GROUP - 1) * slots, sem)

        @pl.when(jnp.logical_not(here))
        def _():
            settle(fetched_ref, GROUP * slots, sem)

        got = []
        for p in owners:
            for s in range(slots):
                l = p * slots + s
                form = form_ref[block_ref[0, l]]
                seen = lax.dot_general(
                    fetched_ref[l], form, (((1,), (1,)), ((), ())), preferred_element_type=F32
                )
                got.append(seen * live_of(p, s))
        first = ((0 if host else half) + t * GROUP) * slots
        for i, term in enumerate(got):
            gath_ref[first + i] = term + summed(gath_ref, 0, first + i)
        return c

    gath_ref[links] = jnp.zeros(gath_ref.shape[1:], F32)
    ret_ref[links] = jnp.zeros(ret_ref.shape[1:], F32)
    by_target = link_chain(target_key, target_key_far, 0)
    by_target.start()

    @pl.when(is_gate)
    def _():
        open_table(planes - 1)
        settle(asked_vmem, planes * (inner - 1), idx_sem.at[2])

    @pl.when(jnp.logical_not(is_gate))
    def _():
        settle(asked_vmem, half, idx_sem.at[2])

    beyond = pl.ds(far, half)
    to_smem = pltpu.make_async_copy(asked_vmem.at[beyond], asked_ref.at[beyond], out_sem.at[2])
    to_smem.start()
    by_target.wait()
    to_smem.wait()
    by_source = link_chain(source_key, source_key_far, 2)
    by_source.start()

    def collect(k, peers, base):
        for s in range(slots):
            i = (base + k) * slots + s
            row = arrived_ref[peers(k) * slots + s]
            ret_ref[i] = row.astype(F32) + summed(ret_ref, 2, i)

    def collect_near(t, c):
        for u in range(GROUP):
            collect(t * GROUP + u, peer, 0)
        return c

    def collect_far(t, c):
        settle(arrived_ref, GROUP * slots, bwd_sem.at[1 + t])
        for u in range(GROUP):
            collect(t * GROUP + u, far_peer, half)
        return c

    def scale(c, carry):
        part_ref[c] = refl_ref[c] / area_ref[pl.ds(c, 1), :]
        return carry

    def far_links(t, c):
        forward(t, c, False)
        return collect_far(t, c)

    for load in loads[6:]:
        load.wait()
    lax.fori_loop(0, clusters, scale, 0, unroll=8)
    lax.fori_loop(0, groups, functools.partial(forward, host=True), 0)
    by_source.wait()
    settle(arrived_ref, (half - 1) * slots, bwd_sem.at[0])
    lax.fori_loop(0, groups, collect_near, 0)
    lax.fori_loop(0, groups, far_links, 0)

    def finish(c, carry):
        gathered, returned = summed(gath_ref, 1, c), summed(ret_ref, 3, c)
        out_ref[c] = em_ref[c] + refl_ref[c] * gathered + part_ref[c] * returned
        return carry

    lax.fori_loop(0, clusters, finish, 0, unroll=8)
    settle(asked_vmem, half, send_sems.at[0])
    settle(bwd_ref, (n - 1) * slots, send_sems.at[1])
    settle(served_ref, (half - 1) * slots, send_sems.at[2])
    settle(rad_ref, share, mirror_sem.at[1])

    @pl.when(is_gate)
    def _():
        settle(asked_vmem, planes * (half - 1), send_sems.at[0])
        settle(served_ref, planes * (half - 1) * slots, send_sems.at[2])


def solution(mesh):
    outer, inner = mesh.shape["gx"], mesh.shape["gy"]
    n = outer * inner

    def shards(
        radiance,
        emission,
        reflectance,
        patch_area,
        form_factor,
        source_index,
        target_index,
        block_index,
        valid_count,
    ):
        clusters, bands, patches = radiance.shape
        links = source_index.shape[1]
        slots = links // n
        tile = (bands, patches)
        hbm = pl.BlockSpec(memory_space=pl.ANY)
        rounds = (n // 2).bit_length() - 2
        return pl.pallas_call(
            functools.partial(exchange, outer, inner),
            out_shape=pltpu.VMEM((clusters,) + tile, F32),
            in_specs=[hbm] * 9,
            out_specs=pl.BlockSpec(memory_space=pltpu.VMEM),
            scratch_shapes=[
                pltpu.SMEM(block_index.shape, jnp.int32),
                pltpu.SMEM(target_index.shape, jnp.int32),
                pltpu.SMEM(valid_count.shape, jnp.int32),
                pltpu.VMEM(source_index.shape, jnp.int32),
                pltpu.VMEM(radiance.shape, BF16),
                pltpu.VMEM(patch_area.shape, F32),
                pltpu.VMEM(form_factor.shape, BF16),
                [pltpu.VMEM((clusters,) + tile, BF16)] * (outer // 2),
                pltpu.VMEM((clusters,) + tile, BF16),
                pltpu.VMEM((links,) + tile, BF16),
                pltpu.VMEM(((1 + outer // 2) * links // 2,) + tile, BF16),
                pltpu.VMEM((links,) + tile, BF16),
                pltpu.VMEM((links,) + tile, BF16),
                pltpu.VMEM((links + 1,) + tile, F32),
                pltpu.VMEM((links + 1,) + tile, F32),
                pltpu.VMEM((clusters,) + tile, F32),
                pltpu.VMEM((clusters,) + tile, F32),
                pltpu.VMEM((clusters,) + tile, F32),
                pltpu.VMEM((n, 1, links), jnp.int32),
                pltpu.SMEM((n, 1, links), jnp.int32),
                pltpu.VMEM((links, patches), jnp.int32),
                pltpu.VMEM((4, 1, links), jnp.int32),
                pltpu.SMEM((4, 1, links), jnp.int32),
                pltpu.SemaphoreType.DMA,
                pltpu.SemaphoreType.DMA((8,)),
                pltpu.SemaphoreType.DMA((3,)),
                pltpu.SemaphoreType.DMA((3,)),
                pltpu.SemaphoreType.REGULAR,
                pltpu.SemaphoreType.REGULAR((rounds,)),
                pltpu.SemaphoreType.DMA((2 + outer // 2,)),
                pltpu.SemaphoreType.DMA((3,)),
                pltpu.SemaphoreType.DMA((1 + n // 2 // GROUP,)),
                pltpu.SemaphoreType.DMA((n // GROUP,)),
            ],
            compiler_params=pltpu.CompilerParams(
                collective_id=0, has_side_effects=True, vmem_limit_bytes=EXCHANGE_MIB * 1024 * 1024
            ),
            name="exchange",
        )(
            block_index,
            target_index,
            valid_count,
            source_index,
            radiance,
            patch_area,
            form_factor,
            emission,
            reflectance,
        )

    spec3 = P(("gx", "gy"), None, None)
    spec2 = P(("gx", "gy"), None)
    return jax.shard_map(
        shards,
        mesh=mesh,
        in_specs=(spec3, spec3, spec3, spec2, spec3, spec2, spec2, spec2, spec2),
        out_specs=spec3,
        check_vma=False,
    )
```

```python
import functools

import jax
import jax.numpy as jnp
from jax import lax
from jax.experimental import pallas as pl
from jax.experimental.pallas import tpu as pltpu
from jax.sharding import PartitionSpec as P

MESH = pl.DeviceIdType.MESH
GROUP = 4
EXCHANGE_MIB = 60
F32 = jnp.float32
BF16 = jnp.bfloat16


def exchange(
    outer,
    inner,
    block_hbm,
    target_hbm,
    count_hbm,
    source_hbm,
    rad_hbm,
    area_hbm,
    form_hbm,
    em_hbm,
    refl_hbm,
    out_ref,
    block_ref,
    target_ref,
    count_ref,
    source_ref,
    rad_ref,
    area_ref,
    form_ref,
    tables,
    weighted_ref,
    bwd_ref,
    served_ref,
    fetched_ref,
    arrived_ref,
    gath_ref,
    ret_ref,
    em_ref,
    refl_ref,
    part_ref,
    asked_vmem,
    asked_ref,
    keys_ref,
    chain_vmem,
    chain_ref,
    form_sem,
    in_sem,
    out_sem,
    send_sems,
    ready_sem,
    round_sem,
    mirror_sem,
    idx_sem,
    bwd_sem,
    rad_sem,
):
    n = outer * inner
    half = n // 2
    gx, gy = lax.axis_index("gx"), lax.axis_index("gy")
    me = gx * inner + gy
    mine = me % half
    near = me // half * half
    far = half - near
    planes = outer // 2
    depth = jnp.where(near == 0, gx, outer - 1 - gx)
    is_gate = depth == planes - 1
    gate = jnp.where(near == 0, planes, planes - 1) * inner + gy
    links = block_ref.shape[1]
    slots = links // n
    clusters = rad_ref.shape[0]
    lanes = keys_ref.shape[1]
    parts = 4
    step = links // parts
    groups = half // GROUP

    def coords(p):
        return (p // inner, p % inner)

    def peer(k):
        return near + (mine + k) % half

    def far_plane(j):
        return jnp.where(near == 0, outer - 1 - j, j) * inner

    def far_peer(k):
        return far_plane(k // inner) + (gy + k) % inner

    loads = [
        pltpu.make_async_copy(src, dst, in_sem.at[i])
        for i, (src, dst) in enumerate(
            (
                (rad_hbm, rad_ref),
                (source_hbm, source_ref),
                (area_hbm, area_ref),
                (block_hbm, block_ref),
                (target_hbm, target_ref),
                (count_hbm, count_ref),
                (em_hbm, em_ref),
                (refl_hbm, refl_ref),
            )
        )
    ]
    forms = [
        pltpu.make_async_copy(
            form_hbm.at[pl.ds(i * step, step)], form_ref.at[pl.ds(i * step, step)], form_sem
        )
        for i in range(parts)
    ]
    for load in loads[:6] + forms + loads[6:]:
        load.start()

    def beside(j):
        bit = 1 << j
        return near + mine + bit - 2 * bit * (mine // bit % 2)

    barrier = pltpu.get_barrier_semaphore()
    bits = half.bit_length() - 1
    for j in range(bits):
        pl.semaphore_signal(barrier, inc=1, device_id=coords(beside(j)), device_id_type=MESH)

    @pl.when(is_gate)
    def _():
        for j in range(planes):
            pl.semaphore_signal(
                barrier, inc=1, device_id=coords(far_plane(j) + gy), device_id_type=MESH
            )

    def settle(ref, rows, sem):
        part = ref.at[pl.ds(0, rows)]
        pltpu.make_async_copy(part, part, sem).wait()

    def idx_copy(to, which, sender=me, src_ref=source_ref):
        return pltpu.make_async_remote_copy(
            src_ref=src_ref,
            dst_ref=asked_vmem.at[sender],
            send_sem=send_sems.at[0],
            recv_sem=idx_sem.at[which],
            device_id=coords(to),
            device_id_type=MESH,
        )

    def bwd_copy(to, which):
        return pltpu.make_async_remote_copy(
            src_ref=bwd_ref.at[pl.ds(to * slots, slots)],
            dst_ref=arrived_ref.at[pl.ds(me * slots, slots)],
            send_sem=send_sems.at[1],
            recv_sem=bwd_sem.at[which],
            device_id=coords(to),
            device_id_type=MESH,
        )

    def rad_copy(to, owner, row, which):
        return pltpu.make_async_remote_copy(
            src_ref=served_ref.at[pl.ds(row * slots, slots)],
            dst_ref=fetched_ref.at[pl.ds(owner * slots, slots)],
            send_sem=send_sems.at[2],
            recv_sem=rad_sem.at[which],
            device_id=coords(to),
            device_id_type=MESH,
        )

    pieces = 4
    share = clusters // pieces
    def across(i, j):
        part = pl.ds(i * share, share)
        return pltpu.make_async_remote_copy(
            src_ref=rad_ref.at[part],
            dst_ref=tables[j].at[part],
            send_sem=mirror_sem.at[0 if i < pieces - 1 else 1],
            recv_sem=mirror_sem.at[2 + j],
            device_id=coords(gate),
            device_id_type=MESH,
        )

    def send_pieces(first, end):
        for j in range(planes):

            @pl.when(depth == j)
            def _():
                for i in range(first, end):
                    across(i, j).start()

    def turn(k):
        return (k + inner) % half

    def send_idx(k, c):
        k = turn(k)

        @pl.when(k != 0)
        def _():
            idx_copy(peer(k), 0).start()

        return c

    def relay_idx(k, c):
        for j in range(planes):
            owner = far_plane(j) + gy
            idx_copy(peer(k), 2, owner, asked_vmem.at[owner]).start()
        return c

    def tell(j):
        pl.semaphore_signal(round_sem.at[j], inc=1, device_id=coords(beside(j)), device_id_type=MESH)

    for load in loads[:2]:
        load.wait()
    pl.semaphore_wait(barrier, bits + 1)
    idx_copy(gate, 1).start()
    send_pieces(0, pieces // 2)
    tell(0)
    asked_vmem[me] = source_ref[...]
    for load in loads[2:6]:
        load.wait()
    for j in range(bits - 2):
        pl.semaphore_wait(round_sem.at[j], 1)
        tell(j + 1)

    def weigh(c, carry):
        area = area_ref[pl.ds(c, 1), :]
        weighted_ref[c] = (area * rad_ref[c].astype(F32)).astype(BF16)
        return carry

    lax.fori_loop(0, clusters, weigh, 0, unroll=8)

    def live_of(p, s):
        return jnp.where(s < count_ref[0, p], 1.0, 0.0).astype(F32)

    pltpu.make_async_copy(form_hbm, form_ref, form_sem).wait()

    def back(p):
        for s in range(slots):
            l = p * slots + s
            form = form_ref[block_ref[0, l]]
            seen = weighted_ref[target_ref[0, l]]
            got = jnp.dot(seen, form, preferred_element_type=F32)
            bwd_ref[l] = (got * live_of(p, s)).astype(BF16)

    def back_near(t, c):
        for u in range(GROUP):
            back(peer(t * GROUP + u))
        return c

    def back_far(t, c):
        for u in range(GROUP):
            back(far_peer(t * GROUP + u))
        return c

    def send_near(k, c):
        k = turn(k)

        @pl.when(k != 0)
        def _():
            bwd_copy(peer(k), 0).start()

        return c

    def send_far(k, c):
        to = jnp.where(k < inner, k, gy + k) % inner
        at = depth * inner + (gy + inner - to) % inner
        bwd_copy(far_plane(k // inner) + to, 1 + at // GROUP).start()
        return c

    def serve(k, c):
        k = turn(k)
        p = peer(k)
        for s in range(slots):
            served_ref[k * slots + s] = rad_ref[asked_ref[p, 0, me * slots + s]]

        @pl.when(k != 0)
        def _():
            rad_copy(p, me, k, (half - k) % half // GROUP).start()

        return c

    def serve_table(k, c, j):
        to = (mine - gy + inner + k) % half
        owner = far_plane(j) + gy
        base = (1 + j) * half + k
        for s in range(slots):
            served_ref[base * slots + s] = tables[j][
                asked_ref[near + to, 0, owner * slots + s]
            ]

        @pl.when(to != mine)
        def _():
            at = j * inner + (gy + inner - k % inner) % inner
            rad_copy(near + to, owner, base, groups + at // GROUP).start()

        return c

    def open_table(j):
        settle(rad_ref, clusters, mirror_sem.at[2 + j])
        lax.fori_loop(0, half, functools.partial(serve_table, j=j), 0)
        owner = far_plane(j) + gy
        base = (1 + j) * half + half - inner + gy
        for s in range(slots):
            fetched_ref[owner * slots + s] = served_ref[base * slots + s]

    lax.fori_loop(0, groups, back_near, 0)
    for s in range(slots):
        arrived_ref[me * slots + s] = bwd_ref[me * slots + s]
    pl.semaphore_wait(round_sem.at[bits - 2], 1)
    lax.fori_loop(0, half, send_idx, 0)

    @pl.when(is_gate)
    def _():
        pl.semaphore_signal(ready_sem, inc=1, device_id=coords(gate), device_id_type=MESH)

    send_pieces(pieces // 2, pieces)
    lax.fori_loop(0, half, send_near, 0)
    lax.fori_loop(0, groups, back_far, 0)

    settle(asked_vmem, half - 1, idx_sem.at[0])
    side = pl.ds(near, half)
    to_smem = pltpu.make_async_copy(asked_vmem.at[side], asked_ref.at[side], out_sem.at[2])
    to_smem.start()
    to_smem.wait()
    lax.fori_loop(0, half, serve, 0)
    for s in range(slots):
        fetched_ref[me * slots + s] = served_ref[s]

    @pl.when(is_gate)
    def _():
        settle(asked_vmem, planes, idx_sem.at[1])
        lax.fori_loop(1, half, relay_idx, 0)

    @pl.when(is_gate)
    def _():
        for j in range(planes - 1):
            open_table(j)

    settle(rad_ref, clusters - share, mirror_sem.at[0])
    pl.semaphore_wait(ready_sem, 1)

    @pl.when(is_gate)
    def _():
        for j in range(1, planes):
            p = near + (mine + j * inner) % half
            pl.semaphore_signal(ready_sem, inc=1, device_id=coords(p), device_id_type=MESH)

    settle(rad_ref, share, mirror_sem.at[1])
    lax.fori_loop(0, half, send_far, 0)

    def link_chain(near_key, far_key, row):
        def fill(k, c, key, base):
            for s in range(slots):
                keys_ref[pl.ds((base + k) * slots + s, 1), :] = jnp.full((1, lanes), key(k, s), jnp.int32)
            return c

        lax.fori_loop(0, half, functools.partial(fill, key=near_key, base=0), 0, unroll=2)
        lax.fori_loop(0, half, functools.partial(fill, key=far_key, base=half), 0, unroll=2)
        keys = keys_ref[...]
        order = lax.broadcasted_iota(jnp.int32, keys.shape, 0)
        lane = lax.broadcasted_iota(jnp.int32, keys.shape, 1)
        for i in range(links // lanes):
            at = lane + i * lanes
            key = jnp.max(jnp.where(order == at, keys, -1), axis=0, keepdims=True)
            before = jnp.max(
                jnp.where((keys == key) & (order < at), order, -1), axis=0, keepdims=True
            )
            chain_vmem[row, :, pl.ds(i * lanes, lanes)] = jnp.where(before < 0, links, before)
        last = jnp.max(jnp.where(keys == lane, order, -1), axis=0, keepdims=True)
        chain_vmem[row + 1, :, pl.ds(0, lanes)] = jnp.where(last < 0, links, last)
        rows = pl.ds(row, 2)
        return pltpu.make_async_copy(chain_vmem.at[rows], chain_ref.at[rows], out_sem.at[row // 2])

    def summed(ref, row, at):
        return ref[chain_ref[row, 0, at]]

    def target_key(k, s):
        return target_ref[0, peer(k) * slots + s]

    def target_key_far(k, s):
        return target_ref[0, far_peer(k) * slots + s]

    def source_key(k, s):
        return asked_ref[peer(k), 0, me * slots + s]

    def source_key_far(k, s):
        return asked_ref[far_peer(k), 0, me * slots + s]

    def forward(t, c, host):
        owners = [(peer if host else far_peer)(t * GROUP + u) for u in range(GROUP)]
        here = (t == 0) if host else is_gate & (t * GROUP % inner == 0)
        sem = rad_sem.at[t if host else groups + t]

        @pl.when(here)
        def _():
            settle(fetched_ref, (GROUP - 1) * slots, sem)

        @pl.when(jnp.logical_not(here))
        def _():
            settle(fetched_ref, GROUP * slots, sem)

        got = []
        for p in owners:
            for s in range(slots):
                l = p * slots + s
                form = form_ref[block_ref[0, l]]
                seen = lax.dot_general(
                    fetched_ref[l], form, (((1,), (1,)), ((), ())), preferred_element_type=F32
                )
                got.append(seen * live_of(p, s))
        first = ((0 if host else half) + t * GROUP) * slots
        for i, term in enumerate(got):
            gath_ref[first + i] = term + summed(gath_ref, 0, first + i)
        return c

    gath_ref[links] = jnp.zeros(gath_ref.shape[1:], F32)
    ret_ref[links] = jnp.zeros(ret_ref.shape[1:], F32)
    by_target = link_chain(target_key, target_key_far, 0)
    by_target.start()

    @pl.when(is_gate)
    def _():
        open_table(planes - 1)
        settle(asked_vmem, planes * (inner - 1), idx_sem.at[2])

    @pl.when(jnp.logical_not(is_gate))
    def _():
        settle(asked_vmem, half, idx_sem.at[2])

    beyond = pl.ds(far, half)
    to_smem = pltpu.make_async_copy(asked_vmem.at[beyond], asked_ref.at[beyond], out_sem.at[2])
    to_smem.start()
    by_target.wait()
    to_smem.wait()
    by_source = link_chain(source_key, source_key_far, 2)
    by_source.start()

    def collect(k, peers, base):
        for s in range(slots):
            i = (base + k) * slots + s
            row = arrived_ref[peers(k) * slots + s]
            ret_ref[i] = row.astype(F32) + summed(ret_ref, 2, i)

    def collect_near(t, c):
        for u in range(GROUP):
            collect(t * GROUP + u, peer, 0)
        return c

    def collect_far(t, c):
        settle(arrived_ref, GROUP * slots, bwd_sem.at[1 + t])
        for u in range(GROUP):
            collect(t * GROUP + u, far_peer, half)
        return c

    def scale(c, carry):
        part_ref[c] = refl_ref[c] / area_ref[pl.ds(c, 1), :]
        return carry

    def far_links(t, c):
        forward(t, c, False)
        return collect_far(t, c)

    for load in loads[6:]:
        load.wait()
    lax.fori_loop(0, clusters, scale, 0, unroll=8)
    lax.fori_loop(0, groups, functools.partial(forward, host=True), 0)
    by_source.wait()
    settle(arrived_ref, (half - 1) * slots, bwd_sem.at[0])
    lax.fori_loop(0, groups, collect_near, 0)
    lax.fori_loop(0, groups, far_links, 0)

    def finish(c, carry):
        gathered, returned = summed(gath_ref, 1, c), summed(ret_ref, 3, c)
        out_ref[c] = em_ref[c] + refl_ref[c] * gathered + part_ref[c] * returned
        return carry

    lax.fori_loop(0, clusters, finish, 0, unroll=8)
    settle(asked_vmem, half, send_sems.at[0])
    settle(bwd_ref, (n - 1) * slots, send_sems.at[1])
    settle(served_ref, (half - 1) * slots, send_sems.at[2])

    @pl.when(is_gate)
    def _():
        settle(asked_vmem, planes * (half - 1), send_sems.at[0])
        settle(served_ref, planes * (half - 1) * slots, send_sems.at[2])


def solution(mesh):
    outer, inner = mesh.shape["gx"], mesh.shape["gy"]
    n = outer * inner

    def shards(
        radiance,
        emission,
        reflectance,
        patch_area,
        form_factor,
        source_index,
        target_index,
        block_index,
        valid_count,
    ):
        clusters, bands, patches = radiance.shape
        links = source_index.shape[1]
        slots = links // n
        tile = (bands, patches)
        hbm = pl.BlockSpec(memory_space=pl.ANY)
        rounds = (n // 2).bit_length() - 2
        return pl.pallas_call(
            functools.partial(exchange, outer, inner),
            out_shape=pltpu.VMEM((clusters,) + tile, F32),
            in_specs=[hbm] * 9,
            out_specs=pl.BlockSpec(memory_space=pltpu.VMEM),
            scratch_shapes=[
                pltpu.SMEM(block_index.shape, jnp.int32),
                pltpu.SMEM(target_index.shape, jnp.int32),
                pltpu.SMEM(valid_count.shape, jnp.int32),
                pltpu.VMEM(source_index.shape, jnp.int32),
                pltpu.VMEM(radiance.shape, BF16),
                pltpu.VMEM(patch_area.shape, F32),
                pltpu.VMEM(form_factor.shape, BF16),
                [pltpu.VMEM((clusters,) + tile, BF16)] * (outer // 2),
                pltpu.VMEM((clusters,) + tile, BF16),
                pltpu.VMEM((links,) + tile, BF16),
                pltpu.VMEM(((1 + outer // 2) * links // 2,) + tile, BF16),
                pltpu.VMEM((links,) + tile, BF16),
                pltpu.VMEM((links,) + tile, BF16),
                pltpu.VMEM((links + 1,) + tile, F32),
                pltpu.VMEM((links + 1,) + tile, F32),
                pltpu.VMEM((clusters,) + tile, F32),
                pltpu.VMEM((clusters,) + tile, F32),
                pltpu.VMEM((clusters,) + tile, F32),
                pltpu.VMEM((n, 1, links), jnp.int32),
                pltpu.SMEM((n, 1, links), jnp.int32),
                pltpu.VMEM((links, patches), jnp.int32),
                pltpu.VMEM((4, 1, links), jnp.int32),
                pltpu.SMEM((4, 1, links), jnp.int32),
                pltpu.SemaphoreType.DMA,
                pltpu.SemaphoreType.DMA((8,)),
                pltpu.SemaphoreType.DMA((3,)),
                pltpu.SemaphoreType.DMA((3,)),
                pltpu.SemaphoreType.REGULAR,
                pltpu.SemaphoreType.REGULAR((rounds,)),
                pltpu.SemaphoreType.DMA((2 + outer // 2,)),
                pltpu.SemaphoreType.DMA((3,)),
                pltpu.SemaphoreType.DMA((1 + n // 2 // GROUP,)),
                pltpu.SemaphoreType.DMA((n // GROUP,)),
            ],
            compiler_params=pltpu.CompilerParams(
                collective_id=0, has_side_effects=True, vmem_limit_bytes=EXCHANGE_MIB * 1024 * 1024
            ),
            name="exchange",
        )(
            block_index,
            target_index,
            valid_count,
            source_index,
            radiance,
            patch_area,
            form_factor,
            emission,
            reflectance,
        )

    spec3 = P(("gx", "gy"), None, None)
    spec2 = P(("gx", "gy"), None)
    return jax.shard_map(
        shards,
        mesh=mesh,
        in_specs=(spec3, spec3, spec3, spec2, spec3, spec2, spec2, spec2, spec2),
        out_specs=spec3,
        check_vma=False,
    )
```

```python
import functools

import jax
import jax.numpy as jnp
from jax import lax
from jax.experimental import pallas as pl
from jax.experimental.pallas import tpu as pltpu
from jax.sharding import PartitionSpec as P

MESH = pl.DeviceIdType.MESH
GROUP = 4
CORES = 2
EXCHANGE_MIB = 60
F32 = jnp.float32
BF16 = jnp.bfloat16


def exchange(
    outer,
    inner,
    block_hbm,
    target_hbm,
    count_hbm,
    source_hbm,
    rad_hbm,
    area_hbm,
    form_hbm,
    em_hbm,
    refl_hbm,
    out_ref,
    block_ref,
    target_ref,
    count_ref,
    source_ref,
    rad_ref,
    area_ref,
    form_ref,
    tables,
    weighted_ref,
    bwd_ref,
    relay_ref,
    turned_ref,
    served_ref,
    fetched_ref,
    arrived_ref,
    gath_ref,
    ret_ref,
    em_ref,
    refl_ref,
    part_ref,
    asked_vmem,
    asked_ref,
    keys_ref,
    chain_vmem,
    chain_ref,
    form_sem,
    in_sem,
    out_sem,
    send_sems,
    ready_sem,
    round_sem,
    mirror_sem,
    idx_sem,
    bwd_sem,
    rad_sem,
):
    n = outer * inner
    half = n // 2
    gx, gy = lax.axis_index("gx"), lax.axis_index("gy")
    me = gx * inner + gy
    mine = me % half
    near = me // half * half
    far = half - near
    planes = outer // 2
    depth = jnp.where(near == 0, gx, outer - 1 - gx)
    is_gate = depth == planes - 1
    gate = jnp.where(near == 0, planes, planes - 1) * inner + gy
    links = block_ref.shape[1]
    slots = links // n
    clusters = rad_ref.shape[0]
    lanes = keys_ref.shape[1]
    parts = 4
    step = links // parts
    groups = half // GROUP

    def coords(p):
        return (p // inner, p % inner)

    def peer(k):
        return near + (mine + k) % half

    def far_plane(j):
        return jnp.where(near == 0, outer - 1 - j, j) * inner

    def far_peer(k):
        return far_plane(k // inner) + (gy + k) % inner

    loads = [
        pltpu.make_async_copy(src, dst, in_sem.at[i])
        for i, (src, dst) in enumerate(
            (
                (rad_hbm, rad_ref),
                (source_hbm, source_ref),
                (area_hbm, area_ref),
                (block_hbm, block_ref),
                (target_hbm, target_ref),
                (count_hbm, count_ref),
                (em_hbm, em_ref),
                (refl_hbm, refl_ref),
            )
        )
    ]
    forms = [
        pltpu.make_async_copy(
            form_hbm.at[pl.ds(i * step, step)], form_ref.at[pl.ds(i * step, step)], form_sem
        )
        for i in range(parts)
    ]
    for load in loads[:6] + forms + loads[6:]:
        load.start()

    def beside(j):
        bit = 1 << j
        return near + mine + bit - 2 * bit * (mine // bit % 2)

    barrier = pltpu.get_barrier_semaphore()
    bits = half.bit_length() - 1
    for j in range(bits):
        pl.semaphore_signal(barrier, inc=1, device_id=coords(beside(j)), device_id_type=MESH)

    @pl.when(is_gate)
    def _():
        for j in range(planes):
            pl.semaphore_signal(
                barrier, inc=1, device_id=coords(far_plane(j) + gy), device_id_type=MESH
            )

    def settle(ref, rows, sem):
        part = ref.at[pl.ds(0, rows)]
        pltpu.make_async_copy(part, part, sem).wait()

    def idx_copy(to, which, sender=me, src_ref=source_ref):
        return pltpu.make_async_remote_copy(
            src_ref=src_ref,
            dst_ref=asked_vmem.at[sender],
            send_sem=send_sems.at[0],
            recv_sem=idx_sem.at[which],
            device_id=coords(to),
            device_id_type=MESH,
        )

    def bwd_copy(to, which):
        return pltpu.make_async_remote_copy(
            src_ref=bwd_ref.at[pl.ds(to * slots, slots)],
            dst_ref=arrived_ref.at[pl.ds(me * slots, slots)],
            send_sem=send_sems.at[1],
            recv_sem=bwd_sem.at[which],
            device_id=coords(to),
            device_id_type=MESH,
        )

    def rad_copy(to, owner, row, which):
        return pltpu.make_async_remote_copy(
            src_ref=served_ref.at[pl.ds(row * slots, slots)],
            dst_ref=fetched_ref.at[pl.ds(owner * slots, slots)],
            send_sem=send_sems.at[2],
            recv_sem=rad_sem.at[which],
            device_id=coords(to),
            device_id_type=MESH,
        )

    pieces = 4
    share = clusters // pieces
    def across(i, j):
        part = pl.ds(i * share, share)
        return pltpu.make_async_remote_copy(
            src_ref=rad_ref.at[part],
            dst_ref=tables[j].at[part],
            send_sem=mirror_sem.at[0 if i < pieces - 1 else 1],
            recv_sem=mirror_sem.at[2 + j],
            device_id=coords(gate),
            device_id_type=MESH,
        )

    def send_pieces(first, end):
        for j in range(planes):

            @pl.when(depth == j)
            def _():
                for i in range(first, end):
                    across(i, j).start()

    def turn(k):
        return (k + inner) % half

    def send_idx(k, c):
        k = turn(k)

        @pl.when(k != 0)
        def _():
            idx_copy(peer(k), 0).start()

        return c

    def relay_idx(k, c):
        for j in range(planes):
            owner = far_plane(j) + gy
            idx_copy(peer(k), 2, owner, asked_vmem.at[owner]).start()
        return c

    def tell(j):
        pl.semaphore_signal(round_sem.at[j], inc=1, device_id=coords(beside(j)), device_id_type=MESH)

    for load in loads[:2]:
        load.wait()
    pl.semaphore_wait(barrier, bits + 1)
    idx_copy(gate, 1).start()
    send_pieces(0, pieces // 2)
    tell(0)
    asked_vmem[me] = source_ref[...]
    for load in loads[2:6]:
        load.wait()
    for j in range(bits - 2):
        pl.semaphore_wait(round_sem.at[j], 1)
        tell(j + 1)

    def weigh(c, carry):
        area = area_ref[pl.ds(c, 1), :]
        weighted_ref[c] = (area * rad_ref[c].astype(F32)).astype(BF16)
        return carry

    lax.fori_loop(0, clusters, weigh, 0, unroll=8)

    def live_of(p, s):
        return jnp.where(s < count_ref[0, p], 1.0, 0.0).astype(F32)

    pltpu.make_async_copy(form_hbm, form_ref, form_sem).wait()

    def back(p):
        for s in range(slots):
            l = p * slots + s
            form = form_ref[block_ref[0, l]]
            seen = weighted_ref[target_ref[0, l]]
            got = jnp.dot(seen, form, preferred_element_type=F32)
            bwd_ref[l] = (got * live_of(p, s)).astype(BF16)

    def back_near(t, c):
        for u in range(GROUP):
            back(peer(t * GROUP + u))
        return c

    def back_far(t, c):
        for u in range(GROUP):
            back(far_peer(t * GROUP + u))
        return c

    def send_near(k, c):
        k = turn(k)

        @pl.when(k != 0)
        def _():
            bwd_copy(peer(k), 0).start()

        return c

    pair = gy // CORES * CORES
    my_depth = CORES - 1 - gy % CORES

    def turn_far(k, c):
        to = (gy + k) % inner
        host = to // CORES * CORES + CORES - 1 - k // inner

        @pl.when(host != gy)
        def _():
            pltpu.make_async_remote_copy(
                src_ref=bwd_ref.at[pl.ds((far_plane(k // inner) + to) * slots, slots)],
                dst_ref=relay_ref.at[to % CORES, pl.ds(gy * slots, slots)],
                send_sem=send_sems.at[1],
                recv_sem=bwd_sem.at[1],
                device_id=(gx, host),
                device_id_type=MESH,
            ).start()

        return c

    def far_copy(core):
        return pltpu.make_async_remote_copy(
            src_ref=relay_ref.at[core],
            dst_ref=arrived_ref.at[pl.ds(gx * inner * slots, inner * slots)],
            send_sem=send_sems.at[3],
            recv_sem=bwd_sem.at[2 + depth],
            device_id=coords(far_plane(my_depth) + pair + core),
            device_id_type=MESH,
        )

    def serve(k, c):
        k = turn(k)
        p = peer(k)
        for s in range(slots):
            served_ref[k * slots + s] = rad_ref[asked_ref[p, 0, me * slots + s]]

        @pl.when(k != 0)
        def _():
            rad_copy(p, me, k, 0).start()

        return c

    def serve_table(k, c, j):
        to = (mine - gy + inner + k) % half
        owner = far_plane(j) + gy
        base = (1 + j) * half + k
        for s in range(slots):
            served_ref[base * slots + s] = tables[j][
                asked_ref[near + to, 0, owner * slots + s]
            ]

        @pl.when(to != mine)
        def _():
            rad_copy(near + to, owner, base, 1 + j).start()

        return c

    def open_table(j):
        settle(rad_ref, clusters, mirror_sem.at[2 + j])
        lax.fori_loop(0, half, functools.partial(serve_table, j=j), 0)
        owner = far_plane(j) + gy
        base = (1 + j) * half + half - inner + gy
        for s in range(slots):
            fetched_ref[owner * slots + s] = served_ref[base * slots + s]

    lax.fori_loop(0, groups, back_far, 0)
    for core in range(CORES):
        for s in range(slots):
            row = (far_plane(my_depth) + pair + core) * slots + s
            relay_ref[core, gy * slots + s] = bwd_ref[row]
    pl.semaphore_wait(round_sem.at[bits - 2], 1)
    lax.fori_loop(0, half, send_idx, 0)

    @pl.when(is_gate)
    def _():
        pl.semaphore_signal(ready_sem, inc=1, device_id=coords(gate), device_id_type=MESH)

    send_pieces(pieces // 2, pieces)
    lax.fori_loop(0, planes * inner, turn_far, 0)
    lax.fori_loop(0, groups, back_near, 0)
    lax.fori_loop(0, half, send_near, 0)
    for s in range(slots):
        arrived_ref[me * slots + s] = bwd_ref[me * slots + s]

    settle(asked_vmem, half - 1, idx_sem.at[0])
    side = pl.ds(near, half)
    to_smem = pltpu.make_async_copy(asked_vmem.at[side], asked_ref.at[side], out_sem.at[2])
    to_smem.start()
    to_smem.wait()
    lax.fori_loop(0, half, serve, 0)
    for s in range(slots):
        fetched_ref[me * slots + s] = served_ref[s]

    @pl.when(is_gate)
    def _():
        settle(asked_vmem, planes, idx_sem.at[1])
        lax.fori_loop(1, half, relay_idx, 0)

    @pl.when(is_gate)
    def _():
        for j in range(planes - 1):
            open_table(j)

    last_core = gy % CORES == CORES - 1

    def let_outer(core):
        for j in range(1, planes):
            p = near + (mine - gy + j * inner) % half + pair + core
            pl.semaphore_signal(ready_sem, inc=1, device_id=coords(p), device_id_type=MESH)

    settle(rad_ref, clusters - share, mirror_sem.at[0])
    pl.semaphore_wait(ready_sem, 1)

    @pl.when(is_gate & last_core)
    def _():
        let_outer(CORES - 1)

    @pl.when(is_gate & last_core & (near == 0))
    def _():
        for core in range(CORES - 1):
            let_outer(core)

    settle(rad_ref, share, mirror_sem.at[1])
    settle(bwd_ref, planes * (inner - 1) * slots, bwd_sem.at[1])
    for core in range(CORES):
        far_copy(core).start()

    def link_chain(near_key, far_key, row):
        def fill(k, c, key, base):
            for s in range(slots):
                keys_ref[pl.ds((base + k) * slots + s, 1), :] = jnp.full((1, lanes), key(k, s), jnp.int32)
            return c

        lax.fori_loop(0, half, functools.partial(fill, key=near_key, base=0), 0, unroll=2)
        lax.fori_loop(0, half, functools.partial(fill, key=far_key, base=half), 0, unroll=2)
        keys = keys_ref[...]
        order = lax.broadcasted_iota(jnp.int32, keys.shape, 0)
        lane = lax.broadcasted_iota(jnp.int32, keys.shape, 1)
        for i in range(links // lanes):
            at = lane + i * lanes
            key = jnp.max(jnp.where(order == at, keys, -1), axis=0, keepdims=True)
            before = jnp.max(
                jnp.where((keys == key) & (order < at), order, -1), axis=0, keepdims=True
            )
            chain_vmem[row, :, pl.ds(i * lanes, lanes)] = jnp.where(before < 0, links, before)
        last = jnp.max(jnp.where(keys == lane, order, -1), axis=0, keepdims=True)
        chain_vmem[row + 1, :, pl.ds(0, lanes)] = jnp.where(last < 0, links, last)
        rows = pl.ds(row, 2)
        return pltpu.make_async_copy(chain_vmem.at[rows], chain_ref.at[rows], out_sem.at[row // 2])

    def summed(ref, row, at):
        return ref[chain_ref[row, 0, at]]

    def target_key(k, s):
        return target_ref[0, peer(k) * slots + s]

    def target_key_far(k, s):
        return target_ref[0, far_peer(k) * slots + s]

    def source_key(k, s):
        return asked_ref[peer(k), 0, me * slots + s]

    def source_key_far(k, s):
        return asked_ref[far_peer(k), 0, me * slots + s]

    def forward(t, c, host):
        owners = [(peer if host else far_peer)(t * GROUP + u) for u in range(GROUP)]
        got = []
        first = ((0 if host else half) + t * GROUP) * slots
        for i, (p, s) in enumerate((p, s) for p in owners for s in range(slots)):
            l = p * slots + s
            if host:
                form = form_ref[block_ref[0, l]]
                seen = lax.dot_general(
                    fetched_ref[l], form, (((1,), (1,)), ((), ())), preferred_element_type=F32
                )
            else:
                form = turned_ref[t * GROUP * slots + i]
                seen = jnp.dot(fetched_ref[l], form, preferred_element_type=F32)
            got.append(seen * live_of(p, s))
        for i, term in enumerate(got):
            gath_ref[first + i] = term + summed(gath_ref, 0, first + i)
        return c

    gath_ref[links] = jnp.zeros(gath_ref.shape[1:], F32)
    ret_ref[links] = jnp.zeros(ret_ref.shape[1:], F32)
    by_target = link_chain(target_key, target_key_far, 0)
    by_target.start()

    @pl.when(is_gate)
    def _():
        open_table(planes - 1)
        settle(asked_vmem, planes * (inner - 1), idx_sem.at[2])

    @pl.when(jnp.logical_not(is_gate))
    def _():
        settle(asked_vmem, half, idx_sem.at[2])

    beyond = pl.ds(far, half)
    to_smem = pltpu.make_async_copy(asked_vmem.at[beyond], asked_ref.at[beyond], out_sem.at[2])
    to_smem.start()
    by_target.wait()
    to_smem.wait()
    by_source = link_chain(source_key, source_key_far, 2)
    by_source.start()

    def collect(k, peers, base):
        for s in range(slots):
            i = (base + k) * slots + s
            row = arrived_ref[peers(k) * slots + s]
            ret_ref[i] = row.astype(F32) + summed(ret_ref, 2, i)

    def collect_near(t, c):
        for u in range(GROUP):
            collect(t * GROUP + u, peer, 0)
        return c

    def collect_far(t, c):
        for u in range(GROUP):
            collect(t * GROUP + u, far_peer, half)
        return c

    def await_served(j):
        @pl.when(is_gate)
        def _():
            settle(fetched_ref, (inner - 1) * slots, rad_sem.at[1 + j])

        @pl.when(jnp.logical_not(is_gate))
        def _():
            settle(fetched_ref, inner * slots, rad_sem.at[1 + j])

    def scale(c, carry):
        part_ref[c] = refl_ref[c] / area_ref[pl.ds(c, 1), :]
        return carry

    for load in loads[6:]:
        load.wait()
    lax.fori_loop(0, clusters, scale, 0, unroll=8)

    @pl.when(is_gate & last_core & (near != 0))
    def _():
        for core in range(CORES - 1):
            let_outer(core)

    settle(fetched_ref, (half - 1) * slots, rad_sem.at[0])
    lax.fori_loop(0, groups, functools.partial(forward, host=True), 0)
    by_source.wait()
    settle(arrived_ref, (half - 1) * slots, bwd_sem.at[0])
    lax.fori_loop(0, groups, collect_near, 0)

    def turn_block(t, c):
        for u in range(GROUP):
            for s in range(slots):
                k = t * GROUP + u
                form = form_ref[block_ref[0, far_peer(k) * slots + s]]
                turned_ref[k * slots + s] = form.T
        return c

    lax.fori_loop(0, groups, turn_block, 0)
    each = inner // GROUP

    def add_forward(j):
        await_served(j)
        lax.fori_loop(j * each, (j + 1) * each, functools.partial(forward, host=False), 0)

    def add_backward(j):
        settle(arrived_ref, inner * slots, bwd_sem.at[2 + j])
        lax.fori_loop(j * each, (j + 1) * each, collect_far, 0)

    def with_gathered(c, carry, to_ref):
        to_ref[c] = em_ref[c] + refl_ref[c] * summed(gath_ref, 1, c)
        return carry

    def with_returned(c, carry, to_ref):
        to_ref[c] = em_ref[c] + part_ref[c] * summed(ret_ref, 3, c)
        return carry

    def blend(step, to_ref):
        lax.fori_loop(0, clusters, functools.partial(step, to_ref=to_ref), 0, unroll=8)

    for j in range(planes - 1):
        add_forward(j)
        add_backward(j)

    forward_first = is_gate | last_core

    @pl.when(forward_first)
    def _():
        add_forward(planes - 1)
        blend(with_gathered, em_ref)
        add_backward(planes - 1)
        blend(with_returned, out_ref)

    @pl.when(jnp.logical_not(forward_first))
    def _():
        add_backward(planes - 1)
        blend(with_returned, em_ref)
        add_forward(planes - 1)
        blend(with_gathered, out_ref)

    settle(asked_vmem, half, send_sems.at[0])
    settle(bwd_ref, (half - 1 + planes * (inner - 1)) * slots, send_sems.at[1])
    settle(bwd_ref, half * slots, send_sems.at[3])
    settle(served_ref, (half - 1) * slots, send_sems.at[2])

    @pl.when(is_gate)
    def _():
        settle(asked_vmem, planes * (half - 1), send_sems.at[0])
        settle(served_ref, planes * (half - 1) * slots, send_sems.at[2])


def solution(mesh):
    outer, inner = mesh.shape["gx"], mesh.shape["gy"]
    n = outer * inner

    def shards(
        radiance,
        emission,
        reflectance,
        patch_area,
        form_factor,
        source_index,
        target_index,
        block_index,
        valid_count,
    ):
        clusters, bands, patches = radiance.shape
        links = source_index.shape[1]
        slots = links // n
        tile = (bands, patches)
        hbm = pl.BlockSpec(memory_space=pl.ANY)
        rounds = (n // 2).bit_length() - 2
        return pl.pallas_call(
            functools.partial(exchange, outer, inner),
            out_shape=pltpu.VMEM((clusters,) + tile, F32),
            in_specs=[hbm] * 9,
            out_specs=pl.BlockSpec(memory_space=pltpu.VMEM),
            scratch_shapes=[
                pltpu.SMEM(block_index.shape, jnp.int32),
                pltpu.SMEM(target_index.shape, jnp.int32),
                pltpu.SMEM(valid_count.shape, jnp.int32),
                pltpu.VMEM(source_index.shape, jnp.int32),
                pltpu.VMEM(radiance.shape, BF16),
                pltpu.VMEM(patch_area.shape, F32),
                pltpu.VMEM(form_factor.shape, BF16),
                [pltpu.VMEM((clusters,) + tile, BF16)] * (outer // 2),
                pltpu.VMEM((clusters,) + tile, BF16),
                pltpu.VMEM((links,) + tile, BF16),
                pltpu.VMEM((CORES, inner * slots) + tile, BF16),
                pltpu.VMEM((links // 2, patches, patches), BF16),
                pltpu.VMEM(((1 + outer // 2) * links // 2,) + tile, BF16),
                pltpu.VMEM((links,) + tile, BF16),
                pltpu.VMEM((links,) + tile, BF16),
                pltpu.VMEM((links + 1,) + tile, F32),
                pltpu.VMEM((links + 1,) + tile, F32),
                pltpu.VMEM((clusters,) + tile, F32),
                pltpu.VMEM((clusters,) + tile, F32),
                pltpu.VMEM((clusters,) + tile, F32),
                pltpu.VMEM((n, 1, links), jnp.int32),
                pltpu.SMEM((n, 1, links), jnp.int32),
                pltpu.VMEM((links, patches), jnp.int32),
                pltpu.VMEM((4, 1, links), jnp.int32),
                pltpu.SMEM((4, 1, links), jnp.int32),
                pltpu.SemaphoreType.DMA,
                pltpu.SemaphoreType.DMA((8,)),
                pltpu.SemaphoreType.DMA((3,)),
                pltpu.SemaphoreType.DMA((4,)),
                pltpu.SemaphoreType.REGULAR,
                pltpu.SemaphoreType.REGULAR((rounds,)),
                pltpu.SemaphoreType.DMA((2 + outer // 2,)),
                pltpu.SemaphoreType.DMA((3,)),
                pltpu.SemaphoreType.DMA((2 + outer // 2,)),
                pltpu.SemaphoreType.DMA((1 + outer // 2,)),
            ],
            compiler_params=pltpu.CompilerParams(
                collective_id=0, has_side_effects=True, vmem_limit_bytes=EXCHANGE_MIB * 1024 * 1024
            ),
            name="exchange",
        )(
            block_index,
            target_index,
            valid_count,
            source_index,
            radiance,
            patch_area,
            form_factor,
            emission,
            reflectance,
        )

    spec3 = P(("gx", "gy"), None, None)
    spec2 = P(("gx", "gy"), None)
    return jax.shard_map(
        shards,
        mesh=mesh,
        in_specs=(spec3, spec3, spec3, spec2, spec3, spec2, spec2, spec2, spec2),
        out_specs=spec3,
        check_vma=False,
    )
```

```python
import functools

import jax
import jax.numpy as jnp
from jax import lax
from jax.experimental import pallas as pl
from jax.experimental.pallas import tpu as pltpu
from jax.sharding import PartitionSpec as P

MESH = pl.DeviceIdType.MESH
GROUP = 4
CORES = 2
EXCHANGE_MIB = 60
F32 = jnp.float32
BF16 = jnp.bfloat16


def exchange(
    outer,
    inner,
    block_hbm,
    target_hbm,
    count_hbm,
    source_hbm,
    rad_hbm,
    area_hbm,
    form_hbm,
    em_hbm,
    refl_hbm,
    out_ref,
    block_ref,
    target_ref,
    count_ref,
    source_ref,
    rad_ref,
    area_ref,
    form_ref,
    tables,
    weighted_ref,
    bwd_ref,
    relay_ref,
    turned_ref,
    served_ref,
    fetched_ref,
    arrived_ref,
    gath_ref,
    ret_ref,
    em_ref,
    refl_ref,
    part_ref,
    asked_vmem,
    asked_ref,
    keys_ref,
    chain_vmem,
    chain_ref,
    form_sem,
    in_sem,
    out_sem,
    send_sems,
    gate_sem,
    ready_sem,
    round_sem,
    mirror_sem,
    idx_sem,
    bwd_sem,
    rad_sem,
):
    n = outer * inner
    half = n // 2
    gx, gy = lax.axis_index("gx"), lax.axis_index("gy")
    me = gx * inner + gy
    mine = me % half
    near = me // half * half
    far = half - near
    planes = outer // 2
    depth = jnp.where(near == 0, gx, outer - 1 - gx)
    is_gate = depth == planes - 1
    first_side = near == 0
    gate = jnp.where(near == 0, planes, planes - 1) * inner + gy
    links = block_ref.shape[1]
    slots = links // n
    clusters = rad_ref.shape[0]
    lanes = keys_ref.shape[1]
    parts = 4
    step = links // parts
    groups = half // GROUP

    def coords(p):
        return (p // inner, p % inner)

    def peer(k):
        return near + (mine + k) % half

    def far_plane(j):
        return jnp.where(near == 0, outer - 1 - j, j) * inner

    def far_peer(k):
        return far_plane(k // inner) + (gy + k) % inner

    loads = [
        pltpu.make_async_copy(src, dst, in_sem.at[i])
        for i, (src, dst) in enumerate(
            (
                (rad_hbm, rad_ref),
                (source_hbm, source_ref),
                (area_hbm, area_ref),
                (block_hbm, block_ref),
                (target_hbm, target_ref),
                (count_hbm, count_ref),
                (em_hbm, em_ref),
                (refl_hbm, refl_ref),
            )
        )
    ]
    forms = [
        pltpu.make_async_copy(
            form_hbm.at[pl.ds(i * step, step)], form_ref.at[pl.ds(i * step, step)], form_sem
        )
        for i in range(parts)
    ]
    for load in loads[:6] + forms + loads[6:]:
        load.start()

    def beside(j):
        bit = 1 << j
        return near + mine + bit - 2 * bit * (mine // bit % 2)

    barrier = pltpu.get_barrier_semaphore()
    bits = half.bit_length() - 1
    for j in range(bits):
        pl.semaphore_signal(barrier, inc=1, device_id=coords(beside(j)), device_id_type=MESH)

    @pl.when(is_gate)
    def _():
        pl.semaphore_signal(barrier, inc=1, device_id=coords(gate), device_id_type=MESH)

    @pl.when(is_gate & first_side)
    def _():
        for j in range(planes - 1):
            pl.semaphore_signal(
                barrier, inc=1, device_id=coords(far_plane(j) + gy), device_id_type=MESH
            )

    def settle(ref, rows, sem):
        part = ref.at[pl.ds(0, rows)]
        pltpu.make_async_copy(part, part, sem).wait()

    def idx_copy(to, which, sender=me, src_ref=source_ref):
        return pltpu.make_async_remote_copy(
            src_ref=src_ref,
            dst_ref=asked_vmem.at[sender],
            send_sem=send_sems.at[0],
            recv_sem=idx_sem.at[which],
            device_id=coords(to),
            device_id_type=MESH,
        )

    def bwd_copy(to, which):
        return pltpu.make_async_remote_copy(
            src_ref=bwd_ref.at[pl.ds(to * slots, slots)],
            dst_ref=arrived_ref.at[pl.ds(me * slots, slots)],
            send_sem=send_sems.at[1],
            recv_sem=bwd_sem.at[which],
            device_id=coords(to),
            device_id_type=MESH,
        )

    def rad_copy(to, owner, row, which):
        return pltpu.make_async_remote_copy(
            src_ref=served_ref.at[pl.ds(row * slots, slots)],
            dst_ref=fetched_ref.at[pl.ds(owner * slots, slots)],
            send_sem=send_sems.at[2],
            recv_sem=rad_sem.at[which],
            device_id=coords(to),
            device_id_type=MESH,
        )

    pieces = 4
    share = clusters // pieces
    def across(i, j):
        part = pl.ds(i * share, share)
        return pltpu.make_async_remote_copy(
            src_ref=rad_ref.at[part],
            dst_ref=tables[j].at[part],
            send_sem=mirror_sem.at[0 if i < pieces - 1 else 1],
            recv_sem=mirror_sem.at[2 + j],
            device_id=coords(gate),
            device_id_type=MESH,
        )

    def send_pieces(first, end):
        for j in range(planes):

            @pl.when(depth == j)
            def _():
                for i in range(first, end):
                    across(i, j).start()

    kinds = (
        (is_gate & first_side, 2),
        (is_gate & jnp.logical_not(first_side), 2),
        (jnp.logical_not(is_gate | first_side), 2),
        (first_side & jnp.logical_not(is_gate), 1),
    )

    def open_cut(which):
        kind, count = which

        @pl.when(kind)
        def _():
            idx_copy(gate, 1).start()
            send_pieces(0, count)

    def turn(k):
        return (k + inner) % half

    def send_idx(k, c):
        k = turn(k)

        @pl.when(k != 0)
        def _():
            idx_copy(peer(k), 0).start()

        return c

    def relay_idx(k, c):
        for j in range(planes):
            owner = far_plane(j) + gy
            idx_copy(peer(k), 2, owner, asked_vmem.at[owner]).start()
        return c

    def tell(j):
        pl.semaphore_signal(round_sem.at[j], inc=1, device_id=coords(beside(j)), device_id_type=MESH)

    for load in loads[:2]:
        load.wait()
    pl.semaphore_wait(barrier, jnp.where(is_gate | (near != 0), bits + 1, bits))

    @pl.when(is_gate & first_side)
    def _():
        for j in range(1, planes):
            p = near + (mine + j * inner) % half
            pl.semaphore_signal(gate_sem, inc=1, device_id=coords(p), device_id_type=MESH)

    for which in kinds[:3]:
        open_cut(which)
    tell(0)
    asked_vmem[me] = source_ref[...]
    for load in loads[2:6]:
        load.wait()
    for j in range(bits - 2):
        pl.semaphore_wait(round_sem.at[j], 1)
        tell(j + 1)
        if j == 0:

            @pl.when(first_side & jnp.logical_not(is_gate))
            def _():
                pl.semaphore_wait(gate_sem, 1)

            open_cut(kinds[3])

    def weigh(c, carry):
        area = area_ref[pl.ds(c, 1), :]
        weighted_ref[c] = (area * rad_ref[c].astype(F32)).astype(BF16)
        return carry

    lax.fori_loop(0, clusters, weigh, 0, unroll=8)

    def live_of(p, s):
        return jnp.where(s < count_ref[0, p], 1.0, 0.0).astype(F32)

    pltpu.make_async_copy(form_hbm, form_ref, form_sem).wait()

    def back(p):
        for s in range(slots):
            l = p * slots + s
            form = form_ref[block_ref[0, l]]
            seen = weighted_ref[target_ref[0, l]]
            got = jnp.dot(seen, form, preferred_element_type=F32)
            bwd_ref[l] = (got * live_of(p, s)).astype(BF16)

    def back_near(t, c):
        for u in range(GROUP):
            back(peer(t * GROUP + u))
        return c

    def back_far(t, c):
        for u in range(GROUP):
            back(far_peer(t * GROUP + u))
        return c

    def send_near(k, c):
        k = turn(k)

        @pl.when(k != 0)
        def _():
            bwd_copy(peer(k), 0).start()

        return c

    pair = gy // CORES * CORES
    my_depth = CORES - 1 - gy % CORES

    def turn_far(k, c):
        to = (gy + k) % inner
        host = to // CORES * CORES + CORES - 1 - k // inner

        @pl.when(host != gy)
        def _():
            pltpu.make_async_remote_copy(
                src_ref=bwd_ref.at[pl.ds((far_plane(k // inner) + to) * slots, slots)],
                dst_ref=relay_ref.at[to % CORES, pl.ds(gy * slots, slots)],
                send_sem=send_sems.at[1],
                recv_sem=bwd_sem.at[1],
                device_id=(gx, host),
                device_id_type=MESH,
            ).start()

        return c

    def far_copy(core):
        return pltpu.make_async_remote_copy(
            src_ref=relay_ref.at[core],
            dst_ref=arrived_ref.at[pl.ds(gx * inner * slots, inner * slots)],
            send_sem=send_sems.at[3],
            recv_sem=bwd_sem.at[2 + depth],
            device_id=coords(far_plane(my_depth) + pair + core),
            device_id_type=MESH,
        )

    def serve(k, c):
        k = turn(k)
        p = peer(k)
        for s in range(slots):
            served_ref[k * slots + s] = rad_ref[asked_ref[p, 0, me * slots + s]]

        @pl.when(k != 0)
        def _():
            rad_copy(p, me, k, 0).start()

        return c

    def serve_table(k, c, j):
        to = (mine - gy + inner + k) % half
        owner = far_plane(j) + gy
        base = (1 + j) * half + k
        for s in range(slots):
            served_ref[base * slots + s] = tables[j][
                asked_ref[near + to, 0, owner * slots + s]
            ]

        @pl.when(to != mine)
        def _():
            rad_copy(near + to, owner, base, 1 + j).start()

        return c

    def open_table(j):
        settle(rad_ref, clusters, mirror_sem.at[2 + j])
        lax.fori_loop(0, half, functools.partial(serve_table, j=j), 0)
        owner = far_plane(j) + gy
        base = (1 + j) * half + half - inner + gy
        for s in range(slots):
            fetched_ref[owner * slots + s] = served_ref[base * slots + s]

    lax.fori_loop(0, groups, back_far, 0)
    for core in range(CORES):
        for s in range(slots):
            row = (far_plane(my_depth) + pair + core) * slots + s
            relay_ref[core, gy * slots + s] = bwd_ref[row]
    pl.semaphore_wait(round_sem.at[bits - 2], 1)
    lax.fori_loop(0, half, send_idx, 0)

    @pl.when(is_gate)
    def _():
        pl.semaphore_signal(ready_sem, inc=1, device_id=coords(gate), device_id_type=MESH)

    for kind, count in kinds:

        @pl.when(kind)
        def _():
            send_pieces(count, pieces)

    lax.fori_loop(0, planes * inner, turn_far, 0)
    lax.fori_loop(0, groups, back_near, 0)
    lax.fori_loop(0, half, send_near, 0)
    for s in range(slots):
        arrived_ref[me * slots + s] = bwd_ref[me * slots + s]

    @pl.when(is_gate & jnp.logical_not(first_side))
    def _():
        settle(asked_vmem, planes, idx_sem.at[1])
        lax.fori_loop(1, half, relay_idx, 0)

    settle(asked_vmem, half - 1, idx_sem.at[0])
    side = pl.ds(near, half)
    to_smem = pltpu.make_async_copy(asked_vmem.at[side], asked_ref.at[side], out_sem.at[2])
    to_smem.start()
    to_smem.wait()
    lax.fori_loop(0, half, serve, 0)
    for s in range(slots):
        fetched_ref[me * slots + s] = served_ref[s]

    @pl.when(is_gate & first_side)
    def _():
        settle(asked_vmem, planes, idx_sem.at[1])
        lax.fori_loop(1, half, relay_idx, 0)

    @pl.when(is_gate)
    def _():
        for j in range(planes - 1):
            open_table(j)

    last_core = gy % CORES == CORES - 1

    def let_outer(core):
        for j in range(1, planes):
            p = near + (mine - gy + j * inner) % half + pair + core
            pl.semaphore_signal(ready_sem, inc=1, device_id=coords(p), device_id_type=MESH)

    settle(rad_ref, clusters - share, mirror_sem.at[0])
    pl.semaphore_wait(ready_sem, 1)

    @pl.when(is_gate & last_core)
    def _():
        let_outer(CORES - 1)

    @pl.when(is_gate & last_core & (near == 0))
    def _():
        for core in range(CORES - 1):
            let_outer(core)

    settle(rad_ref, share, mirror_sem.at[1])
    settle(bwd_ref, planes * (inner - 1) * slots, bwd_sem.at[1])
    for core in range(CORES):
        far_copy(core).start()

    def link_chain(near_key, far_key, row):
        def fill(k, c, key, base):
            for s in range(slots):
                keys_ref[pl.ds((base + k) * slots + s, 1), :] = jnp.full((1, lanes), key(k, s), jnp.int32)
            return c

        lax.fori_loop(0, half, functools.partial(fill, key=near_key, base=0), 0, unroll=2)
        lax.fori_loop(0, half, functools.partial(fill, key=far_key, base=half), 0, unroll=2)
        keys = keys_ref[...]
        order = lax.broadcasted_iota(jnp.int32, keys.shape, 0)
        lane = lax.broadcasted_iota(jnp.int32, keys.shape, 1)
        for i in range(links // lanes):
            at = lane + i * lanes
            key = jnp.max(jnp.where(order == at, keys, -1), axis=0, keepdims=True)
            before = jnp.max(
                jnp.where((keys == key) & (order < at), order, -1), axis=0, keepdims=True
            )
            chain_vmem[row, :, pl.ds(i * lanes, lanes)] = jnp.where(before < 0, links, before)
        last = jnp.max(jnp.where(keys == lane, order, -1), axis=0, keepdims=True)
        chain_vmem[row + 1, :, pl.ds(0, lanes)] = jnp.where(last < 0, links, last)
        rows = pl.ds(row, 2)
        return pltpu.make_async_copy(chain_vmem.at[rows], chain_ref.at[rows], out_sem.at[row // 2])

    def summed(ref, row, at):
        return ref[chain_ref[row, 0, at]]

    def target_key(k, s):
        return target_ref[0, peer(k) * slots + s]

    def target_key_far(k, s):
        return target_ref[0, far_peer(k) * slots + s]

    def source_key(k, s):
        return asked_ref[peer(k), 0, me * slots + s]

    def source_key_far(k, s):
        return asked_ref[far_peer(k), 0, me * slots + s]

    def forward(t, c, host):
        owners = [(peer if host else far_peer)(t * GROUP + u) for u in range(GROUP)]
        got = []
        first = ((0 if host else half) + t * GROUP) * slots
        for i, (p, s) in enumerate((p, s) for p in owners for s in range(slots)):
            l = p * slots + s
            if host:
                form = form_ref[block_ref[0, l]]
                seen = lax.dot_general(
                    fetched_ref[l], form, (((1,), (1,)), ((), ())), preferred_element_type=F32
                )
            else:
                form = turned_ref[t * GROUP * slots + i]
                seen = jnp.dot(fetched_ref[l], form, preferred_element_type=F32)
            got.append(seen * live_of(p, s))
        for i, term in enumerate(got):
            gath_ref[first + i] = term + summed(gath_ref, 0, first + i)
        return c

    gath_ref[links] = jnp.zeros(gath_ref.shape[1:], F32)
    ret_ref[links] = jnp.zeros(ret_ref.shape[1:], F32)
    by_target = link_chain(target_key, target_key_far, 0)
    by_target.start()

    @pl.when(is_gate)
    def _():
        open_table(planes - 1)
        settle(asked_vmem, planes * (inner - 1), idx_sem.at[2])

    @pl.when(jnp.logical_not(is_gate))
    def _():
        settle(asked_vmem, half, idx_sem.at[2])

    beyond = pl.ds(far, half)
    to_smem = pltpu.make_async_copy(asked_vmem.at[beyond], asked_ref.at[beyond], out_sem.at[2])
    to_smem.start()
    by_target.wait()
    to_smem.wait()
    by_source = link_chain(source_key, source_key_far, 2)
    by_source.start()

    def collect(k, peers, base):
        for s in range(slots):
            i = (base + k) * slots + s
            row = arrived_ref[peers(k) * slots + s]
            ret_ref[i] = row.astype(F32) + summed(ret_ref, 2, i)

    def collect_near(t, c):
        for u in range(GROUP):
            collect(t * GROUP + u, peer, 0)
        return c

    def collect_far(t, c):
        for u in range(GROUP):
            collect(t * GROUP + u, far_peer, half)
        return c

    def await_served(j):
        @pl.when(is_gate)
        def _():
            settle(fetched_ref, (inner - 1) * slots, rad_sem.at[1 + j])

        @pl.when(jnp.logical_not(is_gate))
        def _():
            settle(fetched_ref, inner * slots, rad_sem.at[1 + j])

    def scale(c, carry):
        part_ref[c] = refl_ref[c] / area_ref[pl.ds(c, 1), :]
        return carry

    for load in loads[6:]:
        load.wait()
    lax.fori_loop(0, clusters, scale, 0, unroll=8)

    @pl.when(is_gate & last_core & (near != 0))
    def _():
        for core in range(CORES - 1):
            let_outer(core)

    settle(fetched_ref, (half - 1) * slots, rad_sem.at[0])
    lax.fori_loop(0, groups, functools.partial(forward, host=True), 0)
    by_source.wait()
    settle(arrived_ref, (half - 1) * slots, bwd_sem.at[0])
    lax.fori_loop(0, groups, collect_near, 0)

    def turn_block(t, c):
        for u in range(GROUP):
            for s in range(slots):
                k = t * GROUP + u
                form = form_ref[block_ref[0, far_peer(k) * slots + s]]
                turned_ref[k * slots + s] = form.T
        return c

    lax.fori_loop(0, groups, turn_block, 0)
    each = inner // GROUP

    def add_forward(j):
        await_served(j)
        lax.fori_loop(j * each, (j + 1) * each, functools.partial(forward, host=False), 0)

    def add_backward(j):
        settle(arrived_ref, inner * slots, bwd_sem.at[2 + j])
        lax.fori_loop(j * each, (j + 1) * each, collect_far, 0)

    def with_gathered(c, carry, to_ref):
        to_ref[c] = em_ref[c] + refl_ref[c] * summed(gath_ref, 1, c)
        return carry

    def with_returned(c, carry, to_ref):
        to_ref[c] = em_ref[c] + part_ref[c] * summed(ret_ref, 3, c)
        return carry

    def blend(step, to_ref):
        lax.fori_loop(0, clusters, functools.partial(step, to_ref=to_ref), 0, unroll=8)

    for j in range(planes - 1):
        add_forward(j)
        add_backward(j)

    forward_first = is_gate | last_core

    @pl.when(forward_first)
    def _():
        add_forward(planes - 1)
        blend(with_gathered, em_ref)
        add_backward(planes - 1)
        blend(with_returned, out_ref)

    @pl.when(jnp.logical_not(forward_first))
    def _():
        add_backward(planes - 1)
        blend(with_returned, em_ref)
        add_forward(planes - 1)
        blend(with_gathered, out_ref)

    settle(asked_vmem, half, send_sems.at[0])
    settle(bwd_ref, (half - 1 + planes * (inner - 1)) * slots, send_sems.at[1])
    settle(bwd_ref, half * slots, send_sems.at[3])
    settle(served_ref, (half - 1) * slots, send_sems.at[2])

    @pl.when(is_gate)
    def _():
        settle(asked_vmem, planes * (half - 1), send_sems.at[0])
        settle(served_ref, planes * (half - 1) * slots, send_sems.at[2])


def solution(mesh):
    outer, inner = mesh.shape["gx"], mesh.shape["gy"]
    n = outer * inner

    def shards(
        radiance,
        emission,
        reflectance,
        patch_area,
        form_factor,
        source_index,
        target_index,
        block_index,
        valid_count,
    ):
        clusters, bands, patches = radiance.shape
        links = source_index.shape[1]
        slots = links // n
        tile = (bands, patches)
        hbm = pl.BlockSpec(memory_space=pl.ANY)
        rounds = (n // 2).bit_length() - 2
        return pl.pallas_call(
            functools.partial(exchange, outer, inner),
            out_shape=pltpu.VMEM((clusters,) + tile, F32),
            in_specs=[hbm] * 9,
            out_specs=pl.BlockSpec(memory_space=pltpu.VMEM),
            scratch_shapes=[
                pltpu.SMEM(block_index.shape, jnp.int32),
                pltpu.SMEM(target_index.shape, jnp.int32),
                pltpu.SMEM(valid_count.shape, jnp.int32),
                pltpu.VMEM(source_index.shape, jnp.int32),
                pltpu.VMEM(radiance.shape, BF16),
                pltpu.VMEM(patch_area.shape, F32),
                pltpu.VMEM(form_factor.shape, BF16),
                [pltpu.VMEM((clusters,) + tile, BF16)] * (outer // 2),
                pltpu.VMEM((clusters,) + tile, BF16),
                pltpu.VMEM((links,) + tile, BF16),
                pltpu.VMEM((CORES, inner * slots) + tile, BF16),
                pltpu.VMEM((links // 2, patches, patches), BF16),
                pltpu.VMEM(((1 + outer // 2) * links // 2,) + tile, BF16),
                pltpu.VMEM((links,) + tile, BF16),
                pltpu.VMEM((links,) + tile, BF16),
                pltpu.VMEM((links + 1,) + tile, F32),
                pltpu.VMEM((links + 1,) + tile, F32),
                pltpu.VMEM((clusters,) + tile, F32),
                pltpu.VMEM((clusters,) + tile, F32),
                pltpu.VMEM((clusters,) + tile, F32),
                pltpu.VMEM((n, 1, links), jnp.int32),
                pltpu.SMEM((n, 1, links), jnp.int32),
                pltpu.VMEM((links, patches), jnp.int32),
                pltpu.VMEM((4, 1, links), jnp.int32),
                pltpu.SMEM((4, 1, links), jnp.int32),
                pltpu.SemaphoreType.DMA,
                pltpu.SemaphoreType.DMA((8,)),
                pltpu.SemaphoreType.DMA((3,)),
                pltpu.SemaphoreType.DMA((4,)),
                pltpu.SemaphoreType.REGULAR,
                pltpu.SemaphoreType.REGULAR,
                pltpu.SemaphoreType.REGULAR((rounds,)),
                pltpu.SemaphoreType.DMA((2 + outer // 2,)),
                pltpu.SemaphoreType.DMA((3,)),
                pltpu.SemaphoreType.DMA((2 + outer // 2,)),
                pltpu.SemaphoreType.DMA((1 + outer // 2,)),
            ],
            compiler_params=pltpu.CompilerParams(
                collective_id=0, has_side_effects=True, vmem_limit_bytes=EXCHANGE_MIB * 1024 * 1024
            ),
            name="exchange",
        )(
            block_index,
            target_index,
            valid_count,
            source_index,
            radiance,
            patch_area,
            form_factor,
            emission,
            reflectance,
        )

    spec3 = P(("gx", "gy"), None, None)
    spec2 = P(("gx", "gy"), None)
    return jax.shard_map(
        shards,
        mesh=mesh,
        in_specs=(spec3, spec3, spec3, spec2, spec3, spec2, spec2, spec2, spec2),
        out_specs=spec3,
        check_vma=False,
    )
```

```python
import functools

import jax
import jax.numpy as jnp
from jax import lax
from jax.experimental import pallas as pl
from jax.experimental.pallas import tpu as pltpu
from jax.sharding import PartitionSpec as P

MESH = pl.DeviceIdType.MESH
GROUP = 4
CORES = 2
EXCHANGE_MIB = 60
F32 = jnp.float32
BF16 = jnp.bfloat16


def exchange(
    outer,
    inner,
    block_hbm,
    target_hbm,
    count_hbm,
    source_hbm,
    rad_hbm,
    area_hbm,
    form_hbm,
    em_hbm,
    refl_hbm,
    out_ref,
    block_ref,
    target_ref,
    count_ref,
    source_ref,
    rad_ref,
    area_ref,
    form_ref,
    tables,
    weighted_ref,
    bwd_ref,
    relay_ref,
    turned_ref,
    served_ref,
    fetched_ref,
    arrived_ref,
    gath_ref,
    ret_ref,
    em_ref,
    refl_ref,
    part_ref,
    asked_vmem,
    asked_ref,
    keys_ref,
    chain_vmem,
    chain_ref,
    form_sem,
    in_sem,
    out_sem,
    send_sems,
    gate_sem,
    ready_sem,
    round_sem,
    mirror_sem,
    idx_sem,
    bwd_sem,
    rad_sem,
):
    n = outer * inner
    half = n // 2
    gx, gy = lax.axis_index("gx"), lax.axis_index("gy")
    me = gx * inner + gy
    mine = me % half
    near = me // half * half
    far = half - near
    planes = outer // 2
    depth = jnp.where(near == 0, gx, outer - 1 - gx)
    is_gate = depth == planes - 1
    first_side = near == 0
    second_gate = is_gate & jnp.logical_not(first_side)
    second_outer = jnp.logical_not(is_gate | first_side)
    gate = jnp.where(near == 0, planes, planes - 1) * inner + gy
    links = block_ref.shape[1]
    slots = links // n
    clusters = rad_ref.shape[0]
    lanes = keys_ref.shape[1]
    parts = 4
    step = links // parts
    groups = half // GROUP

    def coords(p):
        return (p // inner, p % inner)

    def peer(k):
        return near + (mine + k) % half

    def far_plane(j):
        return jnp.where(near == 0, outer - 1 - j, j) * inner

    def far_peer(k):
        return far_plane(k // inner) + (gy + k) % inner

    loads = [
        pltpu.make_async_copy(src, dst, in_sem.at[i])
        for src, dst, i in (
            (rad_hbm, rad_ref, 0),
            (source_hbm, source_ref, 1),
            (area_hbm, area_ref, 2),
            (block_hbm, block_ref, 3),
            (target_hbm, target_ref, 4),
            (count_hbm, count_ref, 5),
            (em_hbm, em_ref, 6),
            (refl_hbm, refl_ref, 6),
        )
    ]
    forms = [
        pltpu.make_async_copy(
            form_hbm.at[pl.ds(i * step, step)], form_ref.at[pl.ds(i * step, step)], form_sem
        )
        for i in range(parts)
    ]
    for load in loads[:6] + forms + loads[6:]:
        load.start()

    def beside(j):
        bit = 1 << j
        return near + mine + bit - 2 * bit * (mine // bit % 2)

    barrier = pltpu.get_barrier_semaphore()
    bits = half.bit_length() - 1
    for j in range(bits):

        @pl.when(jnp.logical_not(second_gate if j < bits - 1 else second_outer))
        def _():
            pl.semaphore_signal(barrier, inc=1, device_id=coords(beside(j)), device_id_type=MESH)

    @pl.when(is_gate)
    def _():
        pl.semaphore_signal(barrier, inc=1, device_id=coords(gate), device_id_type=MESH)

    @pl.when(is_gate & first_side)
    def _():
        for j in range(planes - 1):
            pl.semaphore_signal(
                barrier, inc=1, device_id=coords(far_plane(j) + gy), device_id_type=MESH
            )

    def settle(ref, rows, sem):
        part = ref.at[pl.ds(0, rows)]
        pltpu.make_async_copy(part, part, sem).wait()

    def idx_copy(to, which, sender=me, src_ref=source_ref):
        return pltpu.make_async_remote_copy(
            src_ref=src_ref,
            dst_ref=asked_vmem.at[sender],
            send_sem=send_sems.at[0],
            recv_sem=idx_sem.at[which],
            device_id=coords(to),
            device_id_type=MESH,
        )

    def bwd_copy(to, which):
        return pltpu.make_async_remote_copy(
            src_ref=bwd_ref.at[pl.ds(to * slots, slots)],
            dst_ref=arrived_ref.at[pl.ds(me * slots, slots)],
            send_sem=send_sems.at[1],
            recv_sem=bwd_sem.at[which],
            device_id=coords(to),
            device_id_type=MESH,
        )

    def rad_copy(to, owner, row, which):
        return pltpu.make_async_remote_copy(
            src_ref=served_ref.at[pl.ds(row * slots, slots)],
            dst_ref=fetched_ref.at[pl.ds(owner * slots, slots)],
            send_sem=send_sems.at[2],
            recv_sem=rad_sem.at[which],
            device_id=coords(to),
            device_id_type=MESH,
        )

    pieces = 4
    share = clusters // pieces
    def across(i, j):
        part = pl.ds(i * share, share)
        return pltpu.make_async_remote_copy(
            src_ref=rad_ref.at[part],
            dst_ref=tables[j].at[part],
            send_sem=mirror_sem.at[0 if i < pieces - 1 else 1],
            recv_sem=mirror_sem.at[2 + j],
            device_id=coords(gate),
            device_id_type=MESH,
        )

    def send_pieces(first, end):
        for j in range(planes):

            @pl.when(depth == j)
            def _():
                for i in range(first, end):
                    across(i, j).start()

    kinds = (
        (is_gate & first_side, 2),
        (is_gate & jnp.logical_not(first_side), 2),
        (jnp.logical_not(is_gate | first_side), 2),
        (first_side & jnp.logical_not(is_gate), 1),
    )

    def open_cut(which):
        kind, count = which

        @pl.when(kind)
        def _():
            idx_copy(gate, 1).start()
            send_pieces(0, count)

    def turn(k):
        return (k + inner) % half

    def send_idx(k, c):
        k = turn(k)

        @pl.when(k != 0)
        def _():
            idx_copy(peer(k), 0).start()

        return c

    def relay_idx(k, c):
        for j in range(planes):
            owner = far_plane(j) + gy
            idx_copy(peer(k), 2, owner, asked_vmem.at[owner]).start()
        return c

    def tell(j):
        pl.semaphore_signal(round_sem.at[j], inc=1, device_id=coords(beside(j)), device_id_type=MESH)

    for load in loads[:2]:
        load.wait()
    greeted = jnp.where(first_side & jnp.logical_not(is_gate), bits, bits + 1)
    pl.semaphore_wait(barrier, jnp.where(second_gate, 1, greeted))

    @pl.when(is_gate & first_side)
    def _():
        for j in range(1, planes):
            p = near + (mine + j * inner) % half
            pl.semaphore_signal(gate_sem, inc=1, device_id=coords(p), device_id_type=MESH)

    for which in kinds[:3]:
        open_cut(which)

    @pl.when(jnp.logical_not(second_gate))
    def _():
        tell(0)

    asked_vmem[me] = source_ref[...]
    for load in loads[2:6]:
        load.wait()
    for j in range(bits - 2):

        @pl.when(jnp.logical_not(second_gate))
        def _():
            pl.semaphore_wait(round_sem.at[j], 1)
            tell(j + 1)

        if j == 0:

            @pl.when(first_side & jnp.logical_not(is_gate))
            def _():
                pl.semaphore_wait(gate_sem, 1)

            open_cut(kinds[3])

    def weigh(c, carry):
        area = area_ref[pl.ds(c, 1), :]
        weighted_ref[c] = (area * rad_ref[c].astype(F32)).astype(BF16)
        return carry

    lax.fori_loop(0, clusters, weigh, 0, unroll=8)

    def live_of(p, s):
        return jnp.where(s < count_ref[0, p], 1.0, 0.0).astype(F32)

    pltpu.make_async_copy(form_hbm, form_ref, form_sem).wait()

    def back(p):
        for s in range(slots):
            l = p * slots + s
            form = form_ref[block_ref[0, l]]
            seen = weighted_ref[target_ref[0, l]]
            got = jnp.dot(seen, form, preferred_element_type=F32)
            bwd_ref[l] = (got * live_of(p, s)).astype(BF16)

    def back_near(t, c):
        for u in range(GROUP):
            back(peer(t * GROUP + u))
        return c

    def back_far(t, c):
        for u in range(GROUP):
            back(far_peer(t * GROUP + u))
        return c

    def send_near(k, c):
        k = turn(k)

        @pl.when(k != 0)
        def _():
            bwd_copy(peer(k), 0).start()

        return c

    pair = gy // CORES * CORES
    my_depth = CORES - 1 - gy % CORES

    def turn_far(k, c):
        to = (gy + k) % inner
        host = to // CORES * CORES + CORES - 1 - k // inner

        @pl.when(host != gy)
        def _():
            pltpu.make_async_remote_copy(
                src_ref=bwd_ref.at[pl.ds((far_plane(k // inner) + to) * slots, slots)],
                dst_ref=relay_ref.at[to % CORES, pl.ds(gy * slots, slots)],
                send_sem=send_sems.at[1],
                recv_sem=bwd_sem.at[1],
                device_id=(gx, host),
                device_id_type=MESH,
            ).start()

        return c

    def far_copy(core, part):
        count = inner // 2 * slots
        return pltpu.make_async_remote_copy(
            src_ref=relay_ref.at[core, pl.ds(part * count, count)],
            dst_ref=arrived_ref.at[pl.ds(gx * inner * slots + part * count, count)],
            send_sem=send_sems.at[3],
            recv_sem=bwd_sem.at[2 + 2 * depth + part],
            device_id=coords(far_plane(my_depth) + pair + core),
            device_id_type=MESH,
        )

    def serve(k, c):
        k = turn(k)
        p = peer(k)
        for s in range(slots):
            served_ref[k * slots + s] = rad_ref[asked_ref[p, 0, me * slots + s]]

        @pl.when(k != 0)
        def _():
            rad_copy(p, me, k, 0).start()

        return c

    def serve_table(k, c, j):
        to = (mine - gy + inner + k) % half
        owner = far_plane(j) + gy
        base = (1 + j) * half + k
        for s in range(slots):
            served_ref[base * slots + s] = tables[j][
                asked_ref[near + to, 0, owner * slots + s]
            ]

        @pl.when(to != mine)
        def _():
            at = (gy + inner - k % inner) % inner
            rad_copy(near + to, owner, base, 1 + 2 * j + at // (inner // 2)).start()

        return c

    def open_table(j):
        settle(rad_ref, clusters, mirror_sem.at[2 + j])
        lax.fori_loop(0, half, functools.partial(serve_table, j=j), 0)
        owner = far_plane(j) + gy
        base = (1 + j) * half + half - inner + gy
        for s in range(slots):
            fetched_ref[owner * slots + s] = served_ref[base * slots + s]

    lax.fori_loop(0, groups, back_far, 0)
    for core in range(CORES):
        for s in range(slots):
            row = (far_plane(my_depth) + pair + core) * slots + s
            relay_ref[core, gy * slots + s] = bwd_ref[row]

    @pl.when(second_gate)
    def _():
        pl.semaphore_wait(gate_sem, 1)

    @pl.when(jnp.logical_not(second_gate))
    def _():
        pl.semaphore_wait(round_sem.at[bits - 2], 1)

    @pl.when(second_outer)
    def _():
        p = coords(beside(bits - 1))
        pl.semaphore_signal(gate_sem, inc=1, device_id=p, device_id_type=MESH)

    lax.fori_loop(0, half, send_idx, 0)

    @pl.when(is_gate)
    def _():
        pl.semaphore_signal(ready_sem, inc=1, device_id=coords(gate), device_id_type=MESH)

    for kind, count in kinds:

        @pl.when(kind)
        def _():
            send_pieces(count, pieces)

    lax.fori_loop(0, planes * inner, turn_far, 0)
    lax.fori_loop(0, groups, back_near, 0)
    lax.fori_loop(0, half, send_near, 0)
    for s in range(slots):
        arrived_ref[me * slots + s] = bwd_ref[me * slots + s]

    @pl.when(is_gate & jnp.logical_not(first_side))
    def _():
        settle(asked_vmem, planes, idx_sem.at[1])
        lax.fori_loop(1, half, relay_idx, 0)

    settle(asked_vmem, half - 1, idx_sem.at[0])
    side = pl.ds(near, half)
    to_smem = pltpu.make_async_copy(asked_vmem.at[side], asked_ref.at[side], out_sem.at[2])
    to_smem.start()
    to_smem.wait()
    lax.fori_loop(0, half, serve, 0)
    for s in range(slots):
        fetched_ref[me * slots + s] = served_ref[s]

    @pl.when(is_gate & first_side)
    def _():
        settle(asked_vmem, planes, idx_sem.at[1])
        lax.fori_loop(1, half, relay_idx, 0)

    @pl.when(is_gate)
    def _():
        for j in range(planes - 1):
            open_table(j)

    last_core = gy % CORES == CORES - 1

    def let_outer(core):
        for j in range(1, planes):
            p = near + (mine - gy + j * inner) % half + pair + core
            pl.semaphore_signal(ready_sem, inc=1, device_id=coords(p), device_id_type=MESH)

    settle(rad_ref, clusters - share, mirror_sem.at[0])
    pl.semaphore_wait(ready_sem, 1)

    @pl.when(is_gate & last_core)
    def _():
        let_outer(CORES - 1)

    @pl.when(is_gate & last_core & (near == 0))
    def _():
        for core in range(CORES - 1):
            let_outer(core)

    settle(rad_ref, share, mirror_sem.at[1])
    settle(bwd_ref, planes * (inner - 1) * slots, bwd_sem.at[1])
    for core in range(CORES):
        for part in range(2):
            far_copy(core, part).start()

    def link_chain(near_key, far_key, row):
        def fill(k, c, key, base):
            for s in range(slots):
                keys_ref[pl.ds((base + k) * slots + s, 1), :] = jnp.full((1, lanes), key(k, s), jnp.int32)
            return c

        lax.fori_loop(0, half, functools.partial(fill, key=near_key, base=0), 0, unroll=2)
        lax.fori_loop(0, half, functools.partial(fill, key=far_key, base=half), 0, unroll=2)
        keys = keys_ref[...]
        order = lax.broadcasted_iota(jnp.int32, keys.shape, 0)
        lane = lax.broadcasted_iota(jnp.int32, keys.shape, 1)
        for i in range(links // lanes):
            at = lane + i * lanes
            key = jnp.max(jnp.where(order == at, keys, -1), axis=0, keepdims=True)
            before = jnp.max(
                jnp.where((keys == key) & (order < at), order, -1), axis=0, keepdims=True
            )
            chain_vmem[row, :, pl.ds(i * lanes, lanes)] = jnp.where(before < 0, links, before)
        last = jnp.max(jnp.where(keys == lane, order, -1), axis=0, keepdims=True)
        chain_vmem[row + 1, :, pl.ds(0, lanes)] = jnp.where(last < 0, links, last)
        rows = pl.ds(row, 2)
        return pltpu.make_async_copy(chain_vmem.at[rows], chain_ref.at[rows], out_sem.at[row // 2])

    def summed(ref, row, at):
        return ref[chain_ref[row, 0, at]]

    def target_key(k, s):
        return target_ref[0, peer(k) * slots + s]

    def target_key_far(k, s):
        return target_ref[0, far_peer(k) * slots + s]

    def far_source(k):
        return far_plane(k // inner) + k % inner

    def source_key(k, s):
        return asked_ref[peer(k), 0, me * slots + s]

    def source_key_far(k, s):
        return asked_ref[far_source(k), 0, me * slots + s]

    def forward(t, c, host):
        owners = [(peer if host else far_peer)(t * GROUP + u) for u in range(GROUP)]
        got = []
        first = ((0 if host else half) + t * GROUP) * slots
        for i, (p, s) in enumerate((p, s) for p in owners for s in range(slots)):
            l = p * slots + s
            if host:
                form = form_ref[block_ref[0, l]]
                seen = lax.dot_general(
                    fetched_ref[l], form, (((1,), (1,)), ((), ())), preferred_element_type=F32
                )
            else:
                form = turned_ref[t * GROUP * slots + i]
                seen = jnp.dot(fetched_ref[l], form, preferred_element_type=F32)
            got.append(seen * live_of(p, s))
        for i, term in enumerate(got):
            gath_ref[first + i] = term + summed(gath_ref, 0, first + i)
        return c

    gath_ref[links] = jnp.zeros(gath_ref.shape[1:], F32)
    ret_ref[links] = jnp.zeros(ret_ref.shape[1:], F32)
    by_target = link_chain(target_key, target_key_far, 0)
    by_target.start()

    @pl.when(is_gate)
    def _():
        open_table(planes - 1)
        settle(asked_vmem, planes * (inner - 1), idx_sem.at[2])

    @pl.when(jnp.logical_not(is_gate))
    def _():
        settle(asked_vmem, half, idx_sem.at[2])

    beyond = pl.ds(far, half)
    to_smem = pltpu.make_async_copy(asked_vmem.at[beyond], asked_ref.at[beyond], out_sem.at[2])
    to_smem.start()
    by_target.wait()
    to_smem.wait()
    by_source = link_chain(source_key, source_key_far, 2)
    by_source.start()

    def collect(k, peers, base):
        for s in range(slots):
            i = (base + k) * slots + s
            row = arrived_ref[peers(k) * slots + s]
            ret_ref[i] = row.astype(F32) + summed(ret_ref, 2, i)

    def collect_near(t, c):
        for u in range(GROUP):
            collect(t * GROUP + u, peer, 0)
        return c

    def collect_far(t, c):
        for u in range(GROUP):
            collect(t * GROUP + u, far_source, half)
        return c

    def await_served(j, part):
        sem = rad_sem.at[1 + 2 * j + part]
        count = inner // 2

        @pl.when(is_gate)
        def _():
            settle(fetched_ref, (count - (part == 0)) * slots, sem)

        @pl.when(jnp.logical_not(is_gate))
        def _():
            settle(fetched_ref, count * slots, sem)

    def scale(c, carry):
        part_ref[c] = refl_ref[c] / area_ref[pl.ds(c, 1), :]
        return carry

    settle(gath_ref, 2 * clusters, in_sem.at[6])
    lax.fori_loop(0, clusters, scale, 0, unroll=8)

    settle(fetched_ref, (half - 1) * slots, rad_sem.at[0])
    lax.fori_loop(0, groups // 2, functools.partial(forward, host=True), 0)

    @pl.when(is_gate & last_core & (near != 0))
    def _():
        for core in range(CORES - 1):
            let_outer(core)

    lax.fori_loop(groups // 2, groups, functools.partial(forward, host=True), 0)
    by_source.wait()
    settle(arrived_ref, (half - 1) * slots, bwd_sem.at[0])
    lax.fori_loop(0, groups, collect_near, 0)

    def turn_block(t, c):
        for u in range(GROUP):
            for s in range(slots):
                k = t * GROUP + u
                form = form_ref[block_ref[0, far_peer(k) * slots + s]]
                turned_ref[k * slots + s] = form.T
        return c

    lax.fori_loop(0, groups, turn_block, 0)
    each = inner // GROUP

    def add_forward(j):
        for part in range(2):
            await_served(j, part)
            first = j * each + part * each // 2
            lax.fori_loop(first, first + each // 2, functools.partial(forward, host=False), 0)

    def add_backward(j):
        for part in range(2):
            settle(arrived_ref, inner // 2 * slots, bwd_sem.at[2 + 2 * j + part])
            first = j * each + part * each // 2
            lax.fori_loop(first, first + each // 2, collect_far, 0)

    def with_gathered(c, carry, to_ref):
        to_ref[c] = em_ref[c] + refl_ref[c] * summed(gath_ref, 1, c)
        return carry

    def with_returned(c, carry, to_ref):
        to_ref[c] = em_ref[c] + part_ref[c] * summed(ret_ref, 3, c)
        return carry

    def blend(step, to_ref):
        lax.fori_loop(0, clusters, functools.partial(step, to_ref=to_ref), 0, unroll=8)

    for j in range(planes - 1):
        add_forward(j)
        add_backward(j)

    forward_first = is_gate

    @pl.when(forward_first)
    def _():
        add_forward(planes - 1)
        blend(with_gathered, em_ref)
        add_backward(planes - 1)
        blend(with_returned, out_ref)

    @pl.when(jnp.logical_not(forward_first))
    def _():
        add_backward(planes - 1)
        blend(with_returned, em_ref)
        add_forward(planes - 1)
        blend(with_gathered, out_ref)

    settle(asked_vmem, half, send_sems.at[0])
    settle(bwd_ref, (half - 1 + planes * (inner - 1)) * slots, send_sems.at[1])
    settle(bwd_ref, half * slots, send_sems.at[3])
    settle(served_ref, (half - 1) * slots, send_sems.at[2])

    @pl.when(is_gate)
    def _():
        settle(asked_vmem, planes * (half - 1), send_sems.at[0])
        settle(served_ref, planes * (half - 1) * slots, send_sems.at[2])


def solution(mesh):
    outer, inner = mesh.shape["gx"], mesh.shape["gy"]
    n = outer * inner

    def shards(
        radiance,
        emission,
        reflectance,
        patch_area,
        form_factor,
        source_index,
        target_index,
        block_index,
        valid_count,
    ):
        clusters, bands, patches = radiance.shape
        links = source_index.shape[1]
        slots = links // n
        tile = (bands, patches)
        hbm = pl.BlockSpec(memory_space=pl.ANY)
        rounds = (n // 2).bit_length() - 2
        return pl.pallas_call(
            functools.partial(exchange, outer, inner),
            out_shape=pltpu.VMEM((clusters,) + tile, F32),
            in_specs=[hbm] * 9,
            out_specs=pl.BlockSpec(memory_space=pltpu.VMEM),
            scratch_shapes=[
                pltpu.SMEM(block_index.shape, jnp.int32),
                pltpu.SMEM(target_index.shape, jnp.int32),
                pltpu.SMEM(valid_count.shape, jnp.int32),
                pltpu.VMEM(source_index.shape, jnp.int32),
                pltpu.VMEM(radiance.shape, BF16),
                pltpu.VMEM(patch_area.shape, F32),
                pltpu.VMEM(form_factor.shape, BF16),
                [pltpu.VMEM((clusters,) + tile, BF16)] * (outer // 2),
                pltpu.VMEM((clusters,) + tile, BF16),
                pltpu.VMEM((links,) + tile, BF16),
                pltpu.VMEM((CORES, inner * slots) + tile, BF16),
                pltpu.VMEM((links // 2, patches, patches), BF16),
                pltpu.VMEM(((1 + outer // 2) * links // 2,) + tile, BF16),
                pltpu.VMEM((links,) + tile, BF16),
                pltpu.VMEM((links,) + tile, BF16),
                pltpu.VMEM((links + 1,) + tile, F32),
                pltpu.VMEM((links + 1,) + tile, F32),
                pltpu.VMEM((clusters,) + tile, F32),
                pltpu.VMEM((clusters,) + tile, F32),
                pltpu.VMEM((clusters,) + tile, F32),
                pltpu.VMEM((n, 1, links), jnp.int32),
                pltpu.SMEM((n, 1, links), jnp.int32),
                pltpu.VMEM((links, patches), jnp.int32),
                pltpu.VMEM((4, 1, links), jnp.int32),
                pltpu.SMEM((4, 1, links), jnp.int32),
                pltpu.SemaphoreType.DMA,
                pltpu.SemaphoreType.DMA((7,)),
                pltpu.SemaphoreType.DMA((3,)),
                pltpu.SemaphoreType.DMA((4,)),
                pltpu.SemaphoreType.REGULAR,
                pltpu.SemaphoreType.REGULAR,
                pltpu.SemaphoreType.REGULAR((rounds,)),
                pltpu.SemaphoreType.DMA((2 + outer // 2,)),
                pltpu.SemaphoreType.DMA((3,)),
                pltpu.SemaphoreType.DMA((2 + outer,)),
                pltpu.SemaphoreType.DMA((1 + outer,)),
            ],
            compiler_params=pltpu.CompilerParams(
                collective_id=0, has_side_effects=True, vmem_limit_bytes=EXCHANGE_MIB * 1024 * 1024
            ),
            name="exchange",
        )(
            block_index,
            target_index,
            valid_count,
            source_index,
            radiance,
            patch_area,
            form_factor,
            emission,
            reflectance,
        )

    spec3 = P(("gx", "gy"), None, None)
    spec2 = P(("gx", "gy"), None)
    return jax.shard_map(
        shards,
        mesh=mesh,
        in_specs=(spec3, spec3, spec3, spec2, spec3, spec2, spec2, spec2, spec2),
        out_specs=spec3,
        check_vma=False,
    )
```

```python
import functools

import jax
import jax.numpy as jnp
from jax import lax
from jax.experimental import pallas as pl
from jax.experimental.pallas import tpu as pltpu
from jax.sharding import PartitionSpec as P

MESH = pl.DeviceIdType.MESH
GROUP = 4
CORES = 2
EXCHANGE_MIB = 60
F32 = jnp.float32
BF16 = jnp.bfloat16


def exchange(
    outer,
    inner,
    block_hbm,
    target_hbm,
    count_hbm,
    source_hbm,
    rad_hbm,
    area_hbm,
    form_hbm,
    em_hbm,
    refl_hbm,
    out_ref,
    block_ref,
    target_ref,
    count_ref,
    source_ref,
    rad_ref,
    area_ref,
    form_ref,
    tables,
    weighted_ref,
    bwd_ref,
    relay_ref,
    turned_ref,
    served_ref,
    fetched_ref,
    arrived_ref,
    gath_ref,
    ret_ref,
    em_ref,
    refl_ref,
    part_ref,
    asked_vmem,
    asked_ref,
    keys_ref,
    chain_vmem,
    chain_ref,
    form_sem,
    in_sem,
    out_sem,
    send_sems,
    gate_sem,
    ready_sem,
    round_sem,
    mirror_sem,
    idx_sem,
    bwd_sem,
    rad_sem,
):
    n = outer * inner
    half = n // 2
    gx, gy = lax.axis_index("gx"), lax.axis_index("gy")
    me = gx * inner + gy
    mine = me % half
    near = me // half * half
    far = half - near
    planes = outer // 2
    depth = jnp.where(near == 0, gx, outer - 1 - gx)
    is_gate = depth == planes - 1
    first_side = near == 0
    second_gate = is_gate & jnp.logical_not(first_side)
    second_outer = jnp.logical_not(is_gate | first_side)
    gate = jnp.where(near == 0, planes, planes - 1) * inner + gy
    links = block_ref.shape[1]
    slots = links // n
    clusters = rad_ref.shape[0]
    lanes = keys_ref.shape[1]
    parts = 4
    step = links // parts
    groups = half // GROUP

    def coords(p):
        return (p // inner, p % inner)

    def peer(k):
        return near + (mine + k) % half

    def far_plane(j):
        return jnp.where(near == 0, outer - 1 - j, j) * inner

    def far_peer(k):
        return far_plane(k // inner) + (gy + k) % inner

    loads = [
        pltpu.make_async_copy(src, dst, in_sem.at[i])
        for src, dst, i in (
            (rad_hbm, rad_ref, 0),
            (source_hbm, source_ref, 1),
            (area_hbm, area_ref, 2),
            (block_hbm, block_ref, 3),
            (target_hbm, target_ref, 4),
            (count_hbm, count_ref, 5),
            (em_hbm, em_ref, 6),
            (refl_hbm, refl_ref, 6),
        )
    ]
    forms = [
        pltpu.make_async_copy(
            form_hbm.at[pl.ds(i * step, step)], form_ref.at[pl.ds(i * step, step)], form_sem
        )
        for i in range(parts)
    ]
    for load in loads[:6] + forms + loads[6:]:
        load.start()

    def beside(j):
        bit = 1 << j
        return near + mine + bit - 2 * bit * (mine // bit % 2)

    barrier = pltpu.get_barrier_semaphore()
    bits = half.bit_length() - 1
    for j in range(bits):

        @pl.when(jnp.logical_not(second_gate if j < bits - 1 else second_outer))
        def _():
            pl.semaphore_signal(barrier, inc=1, device_id=coords(beside(j)), device_id_type=MESH)

    @pl.when(is_gate)
    def _():
        pl.semaphore_signal(barrier, inc=1, device_id=coords(gate), device_id_type=MESH)

    @pl.when(is_gate & first_side)
    def _():
        for j in range(planes - 1):
            pl.semaphore_signal(
                barrier, inc=1, device_id=coords(far_plane(j) + gy), device_id_type=MESH
            )

    def settle(ref, rows, sem):
        part = ref.at[pl.ds(0, rows)]
        pltpu.make_async_copy(part, part, sem).wait()

    def idx_copy(to, which, sender=me, src_ref=source_ref):
        return pltpu.make_async_remote_copy(
            src_ref=src_ref,
            dst_ref=asked_vmem.at[sender],
            send_sem=send_sems.at[0],
            recv_sem=idx_sem.at[which],
            device_id=coords(to),
            device_id_type=MESH,
        )

    def bwd_copy(to, which):
        return pltpu.make_async_remote_copy(
            src_ref=bwd_ref.at[pl.ds(to * slots, slots)],
            dst_ref=arrived_ref.at[pl.ds(me * slots, slots)],
            send_sem=send_sems.at[1],
            recv_sem=bwd_sem.at[which],
            device_id=coords(to),
            device_id_type=MESH,
        )

    def rad_copy(to, owner, row, which):
        return pltpu.make_async_remote_copy(
            src_ref=served_ref.at[pl.ds(row * slots, slots)],
            dst_ref=fetched_ref.at[pl.ds(owner * slots, slots)],
            send_sem=send_sems.at[2],
            recv_sem=rad_sem.at[which],
            device_id=coords(to),
            device_id_type=MESH,
        )

    pieces = 4
    share = clusters // pieces
    def across(i, j):
        part = pl.ds(i * share, share)
        return pltpu.make_async_remote_copy(
            src_ref=rad_ref.at[part],
            dst_ref=tables[j].at[part],
            send_sem=mirror_sem.at[0 if i < pieces - 1 else 1],
            recv_sem=mirror_sem.at[2 + j],
            device_id=coords(gate),
            device_id_type=MESH,
        )

    def send_pieces(first, end):
        for j in range(planes):

            @pl.when(depth == j)
            def _():
                for i in range(first, end):
                    across(i, j).start()

    kinds = (
        (is_gate & first_side, 2),
        (is_gate & jnp.logical_not(first_side), 2),
        (jnp.logical_not(is_gate | first_side), 2),
        (first_side & jnp.logical_not(is_gate), 1),
    )

    def open_cut(which):
        kind, count = which

        @pl.when(kind)
        def _():
            idx_copy(gate, 1).start()
            send_pieces(0, count)

    def turn(k):
        return (k + inner) % half

    def send_idx(k, c):
        k = turn(k)

        @pl.when(k != 0)
        def _():
            idx_copy(peer(k), 0).start()

        return c

    def relay_idx(k, c):
        for j in range(planes):
            owner = far_plane(j) + gy
            idx_copy(peer(k), 2, owner, asked_vmem.at[owner]).start()
        return c

    def tell(j):
        pl.semaphore_signal(round_sem.at[j], inc=1, device_id=coords(beside(j)), device_id_type=MESH)

    for load in loads[:2]:
        load.wait()
    greeted = jnp.where(first_side & jnp.logical_not(is_gate), bits, bits + 1)
    pl.semaphore_wait(barrier, jnp.where(second_gate, 1, greeted))

    @pl.when(is_gate & first_side)
    def _():
        for j in range(1, planes):
            p = near + (mine + j * inner) % half
            pl.semaphore_signal(gate_sem, inc=1, device_id=coords(p), device_id_type=MESH)

    for which in kinds[:3]:
        open_cut(which)

    @pl.when(jnp.logical_not(second_gate))
    def _():
        tell(0)

    asked_vmem[me] = source_ref[...]
    for load in loads[2:6]:
        load.wait()
    for j in range(bits - 2):

        @pl.when(jnp.logical_not(second_gate))
        def _():
            pl.semaphore_wait(round_sem.at[j], 1)
            tell(j + 1)

        if j == 0:

            @pl.when(first_side & jnp.logical_not(is_gate))
            def _():
                pl.semaphore_wait(gate_sem, 1)

            open_cut(kinds[3])

    def weigh(c, carry):
        area = area_ref[pl.ds(c, 1), :]
        weighted_ref[c] = (area * rad_ref[c].astype(F32)).astype(BF16)
        return carry

    lax.fori_loop(0, clusters, weigh, 0, unroll=8)

    def live_of(p, s):
        return jnp.where(s < count_ref[0, p], 1.0, 0.0).astype(F32)

    pltpu.make_async_copy(form_hbm, form_ref, form_sem).wait()

    def back(p):
        for s in range(slots):
            l = p * slots + s
            form = form_ref[block_ref[0, l]]
            seen = weighted_ref[target_ref[0, l]]
            got = jnp.dot(seen, form, preferred_element_type=F32)
            bwd_ref[l] = (got * live_of(p, s)).astype(BF16)

    def back_near(t, c):
        for u in range(GROUP):
            back(peer(t * GROUP + u))
        return c

    def back_far(t, c):
        for u in range(GROUP):
            back(far_peer(t * GROUP + u))
        return c

    def send_near(k, c):
        k = turn(k)

        @pl.when(k != 0)
        def _():
            bwd_copy(peer(k), 0).start()

        return c

    pair = gy // CORES * CORES
    my_depth = CORES - 1 - gy % CORES

    def turn_far(k, c):
        to = (gy + k) % inner
        host = to // CORES * CORES + CORES - 1 - k // inner

        @pl.when(host != gy)
        def _():
            pltpu.make_async_remote_copy(
                src_ref=bwd_ref.at[pl.ds((far_plane(k // inner) + to) * slots, slots)],
                dst_ref=relay_ref.at[to % CORES, pl.ds(gy * slots, slots)],
                send_sem=send_sems.at[1],
                recv_sem=bwd_sem.at[1],
                device_id=(gx, host),
                device_id_type=MESH,
            ).start()

        return c

    def far_copy(core, part):
        count = inner // 2 * slots
        return pltpu.make_async_remote_copy(
            src_ref=relay_ref.at[core, pl.ds(part * count, count)],
            dst_ref=arrived_ref.at[pl.ds(gx * inner * slots + part * count, count)],
            send_sem=send_sems.at[3],
            recv_sem=bwd_sem.at[2 + 2 * depth + part],
            device_id=coords(far_plane(my_depth) + pair + core),
            device_id_type=MESH,
        )

    def serve(k, c):
        k = turn(k)
        p = peer(k)
        for s in range(slots):
            served_ref[k * slots + s] = rad_ref[asked_ref[p, 0, me * slots + s]]

        @pl.when(k != 0)
        def _():
            rad_copy(p, me, k, 0).start()

        return c

    def serve_table(k, c, j):
        to = (mine - gy + inner + k) % half
        owner = far_plane(j) + gy
        base = (1 + j) * half + k
        for s in range(slots):
            served_ref[base * slots + s] = tables[j][
                asked_ref[near + to, 0, owner * slots + s]
            ]

        @pl.when(to != mine)
        def _():
            at = (gy + inner - k % inner) % inner
            rad_copy(near + to, owner, base, 1 + 2 * j + at // (inner // 2)).start()

        return c

    def open_table(j):
        settle(rad_ref, clusters, mirror_sem.at[2 + j])
        lax.fori_loop(0, half, functools.partial(serve_table, j=j), 0)
        owner = far_plane(j) + gy
        base = (1 + j) * half + half - inner + gy
        for s in range(slots):
            fetched_ref[owner * slots + s] = served_ref[base * slots + s]

    lax.fori_loop(0, groups, back_far, 0)
    for core in range(CORES):
        for s in range(slots):
            row = (far_plane(my_depth) + pair + core) * slots + s
            relay_ref[core, gy * slots + s] = bwd_ref[row]

    @pl.when(second_gate)
    def _():
        pl.semaphore_wait(gate_sem, 1)

    @pl.when(jnp.logical_not(second_gate))
    def _():
        pl.semaphore_wait(round_sem.at[bits - 2], 1)

    @pl.when(second_outer)
    def _():
        p = coords(beside(bits - 1))
        pl.semaphore_signal(gate_sem, inc=1, device_id=p, device_id_type=MESH)

    lax.fori_loop(0, half, send_idx, 0)

    @pl.when(is_gate)
    def _():
        pl.semaphore_signal(ready_sem, inc=1, device_id=coords(gate), device_id_type=MESH)

    for kind, count in kinds:

        @pl.when(kind)
        def _():
            send_pieces(count, pieces)

    lax.fori_loop(0, planes * inner, turn_far, 0)
    lax.fori_loop(0, groups, back_near, 0)
    lax.fori_loop(0, half, send_near, 0)
    for s in range(slots):
        arrived_ref[me * slots + s] = bwd_ref[me * slots + s]

    @pl.when(is_gate & jnp.logical_not(first_side))
    def _():
        settle(asked_vmem, planes, idx_sem.at[1])
        lax.fori_loop(1, half, relay_idx, 0)

    settle(asked_vmem, half - 1, idx_sem.at[0])
    side = pl.ds(near, half)
    to_smem = pltpu.make_async_copy(asked_vmem.at[side], asked_ref.at[side], out_sem.at[2])
    to_smem.start()
    to_smem.wait()
    lax.fori_loop(0, half, serve, 0)
    for s in range(slots):
        fetched_ref[me * slots + s] = served_ref[s]

    @pl.when(is_gate & first_side)
    def _():
        settle(asked_vmem, planes, idx_sem.at[1])
        lax.fori_loop(1, half, relay_idx, 0)

    @pl.when(is_gate)
    def _():
        for j in range(planes - 1):
            open_table(j)

    last_core = gy % CORES == CORES - 1

    def let_outer(core):
        for j in range(1, planes):
            p = near + (mine - gy + j * inner) % half + pair + core
            pl.semaphore_signal(ready_sem, inc=1, device_id=coords(p), device_id_type=MESH)

    settle(rad_ref, clusters - share, mirror_sem.at[0])
    pl.semaphore_wait(ready_sem, 1)

    @pl.when(is_gate & last_core)
    def _():
        let_outer(CORES - 1)

    @pl.when(is_gate & last_core & (near == 0))
    def _():
        for core in range(CORES - 1):
            let_outer(core)

    settle(rad_ref, share, mirror_sem.at[1])
    settle(bwd_ref, planes * (inner - 1) * slots, bwd_sem.at[1])
    for core in range(CORES):
        for part in range(2):
            far_copy(core, part).start()

    def link_chain(near_key, far_key, row):
        def fill(k, c, key, base):
            for s in range(slots):
                keys_ref[pl.ds((base + k) * slots + s, 1), :] = jnp.full((1, lanes), key(k, s), jnp.int32)
            return c

        lax.fori_loop(0, half, functools.partial(fill, key=near_key, base=0), 0, unroll=2)
        lax.fori_loop(0, half, functools.partial(fill, key=far_key, base=half), 0, unroll=2)
        keys = keys_ref[...]
        order = lax.broadcasted_iota(jnp.int32, keys.shape, 0)
        lane = lax.broadcasted_iota(jnp.int32, keys.shape, 1)
        for i in range(links // lanes):
            at = lane + i * lanes
            key = jnp.max(jnp.where(order == at, keys, -1), axis=0, keepdims=True)
            before = jnp.max(
                jnp.where((keys == key) & (order < at), order, -1), axis=0, keepdims=True
            )
            chain_vmem[row, :, pl.ds(i * lanes, lanes)] = jnp.where(before < 0, links, before)
        last = jnp.max(jnp.where(keys == lane, order, -1), axis=0, keepdims=True)
        chain_vmem[row + 1, :, pl.ds(0, lanes)] = jnp.where(last < 0, links, last)
        rows = pl.ds(row, 2)
        return pltpu.make_async_copy(chain_vmem.at[rows], chain_ref.at[rows], out_sem.at[row // 2])

    def summed(ref, row, at):
        return ref[chain_ref[row, 0, at]]

    def target_key(k, s):
        return target_ref[0, peer(k) * slots + s]

    def target_key_far(k, s):
        return target_ref[0, far_peer(k) * slots + s]

    def far_source(k):
        return far_plane(k // inner) + k % inner

    def source_key(k, s):
        return asked_ref[peer(k), 0, me * slots + s]

    def source_key_far(k, s):
        return asked_ref[far_source(k), 0, me * slots + s]

    def forward(t, c, host):
        owners = [(peer if host else far_peer)(t * GROUP + u) for u in range(GROUP)]
        got = []
        first = ((0 if host else half) + t * GROUP) * slots
        for i, (p, s) in enumerate((p, s) for p in owners for s in range(slots)):
            l = p * slots + s
            if host:
                form = form_ref[block_ref[0, l]]
                seen = lax.dot_general(
                    fetched_ref[l], form, (((1,), (1,)), ((), ())), preferred_element_type=F32
                )
            else:
                form = turned_ref[t * GROUP * slots + i]
                seen = jnp.dot(fetched_ref[l], form, preferred_element_type=F32)
            got.append(seen * live_of(p, s))
        for i, term in enumerate(got):
            gath_ref[first + i] = term + summed(gath_ref, 0, first + i)
        return c

    gath_ref[links] = jnp.zeros(gath_ref.shape[1:], F32)
    ret_ref[links] = jnp.zeros(ret_ref.shape[1:], F32)
    by_target = link_chain(target_key, target_key_far, 0)
    by_target.start()

    @pl.when(is_gate)
    def _():
        open_table(planes - 1)
        settle(asked_vmem, planes * (inner - 1), idx_sem.at[2])

    @pl.when(jnp.logical_not(is_gate))
    def _():
        settle(asked_vmem, half, idx_sem.at[2])

    beyond = pl.ds(far, half)
    to_smem = pltpu.make_async_copy(asked_vmem.at[beyond], asked_ref.at[beyond], out_sem.at[2])
    to_smem.start()
    by_target.wait()
    to_smem.wait()
    by_source = link_chain(source_key, source_key_far, 2)
    by_source.start()

    def collect(k, peers, base):
        for s in range(slots):
            i = (base + k) * slots + s
            row = arrived_ref[peers(k) * slots + s]
            ret_ref[i] = row.astype(F32) + summed(ret_ref, 2, i)

    def collect_near(t, c):
        for u in range(GROUP):
            collect(t * GROUP + u, peer, 0)
        return c

    def collect_far(t, c):
        for u in range(GROUP):
            collect(t * GROUP + u, far_source, half)
        return c

    def await_served(j, part):
        sem = rad_sem.at[1 + 2 * j + part]
        count = inner // 2

        @pl.when(is_gate)
        def _():
            settle(fetched_ref, (count - (part == 0)) * slots, sem)

        @pl.when(jnp.logical_not(is_gate))
        def _():
            settle(fetched_ref, count * slots, sem)

    def scale(c, carry):
        part_ref[c] = refl_ref[c] / area_ref[pl.ds(c, 1), :]
        return carry

    settle(gath_ref, 2 * clusters, in_sem.at[6])
    lax.fori_loop(0, clusters, scale, 0, unroll=8)

    @pl.when(is_gate & last_core & (near != 0))
    def _():
        for core in range(CORES - 1):
            let_outer(core)

    settle(fetched_ref, (half - 1) * slots, rad_sem.at[0])
    lax.fori_loop(0, groups, functools.partial(forward, host=True), 0)
    by_source.wait()
    settle(arrived_ref, (half - 1) * slots, bwd_sem.at[0])
    lax.fori_loop(0, groups, collect_near, 0)

    def turn_block(t, c):
        for u in range(GROUP):
            for s in range(slots):
                k = t * GROUP + u
                form = form_ref[block_ref[0, far_peer(k) * slots + s]]
                turned_ref[k * slots + s] = form.T
        return c

    lax.fori_loop(0, groups, turn_block, 0)
    each = inner // GROUP

    def add_forward(j):
        for part in range(2):
            await_served(j, part)
            first = j * each + part * each // 2
            lax.fori_loop(first, first + each // 2, functools.partial(forward, host=False), 0)

    def add_backward(j):
        for part in range(2):
            settle(arrived_ref, inner // 2 * slots, bwd_sem.at[2 + 2 * j + part])
            first = j * each + part * each // 2
            lax.fori_loop(first, first + each // 2, collect_far, 0)

    def with_gathered(c, carry, to_ref):
        to_ref[c] = em_ref[c] + refl_ref[c] * summed(gath_ref, 1, c)
        return carry

    def with_returned(c, carry, to_ref):
        to_ref[c] = em_ref[c] + part_ref[c] * summed(ret_ref, 3, c)
        return carry

    def blend(step, to_ref):
        lax.fori_loop(0, clusters, functools.partial(step, to_ref=to_ref), 0, unroll=8)

    for j in range(planes - 1):
        add_forward(j)
        add_backward(j)

    forward_first = is_gate | last_core

    @pl.when(forward_first)
    def _():
        add_forward(planes - 1)
        blend(with_gathered, em_ref)
        add_backward(planes - 1)
        blend(with_returned, out_ref)

    @pl.when(jnp.logical_not(forward_first))
    def _():
        add_backward(planes - 1)
        blend(with_returned, em_ref)
        add_forward(planes - 1)
        blend(with_gathered, out_ref)

    settle(asked_vmem, half, send_sems.at[0])
    settle(bwd_ref, (half - 1 + planes * (inner - 1)) * slots, send_sems.at[1])
    settle(bwd_ref, half * slots, send_sems.at[3])
    settle(served_ref, (half - 1) * slots, send_sems.at[2])

    @pl.when(is_gate)
    def _():
        settle(asked_vmem, planes * (half - 1), send_sems.at[0])
        settle(served_ref, planes * (half - 1) * slots, send_sems.at[2])


def solution(mesh):
    outer, inner = mesh.shape["gx"], mesh.shape["gy"]
    n = outer * inner

    def shards(
        radiance,
        emission,
        reflectance,
        patch_area,
        form_factor,
        source_index,
        target_index,
        block_index,
        valid_count,
    ):
        clusters, bands, patches = radiance.shape
        links = source_index.shape[1]
        slots = links // n
        tile = (bands, patches)
        hbm = pl.BlockSpec(memory_space=pl.ANY)
        rounds = (n // 2).bit_length() - 2
        return pl.pallas_call(
            functools.partial(exchange, outer, inner),
            out_shape=pltpu.VMEM((clusters,) + tile, F32),
            in_specs=[hbm] * 9,
            out_specs=pl.BlockSpec(memory_space=pltpu.VMEM),
            scratch_shapes=[
                pltpu.SMEM(block_index.shape, jnp.int32),
                pltpu.SMEM(target_index.shape, jnp.int32),
                pltpu.SMEM(valid_count.shape, jnp.int32),
                pltpu.VMEM(source_index.shape, jnp.int32),
                pltpu.VMEM(radiance.shape, BF16),
                pltpu.VMEM(patch_area.shape, F32),
                pltpu.VMEM(form_factor.shape, BF16),
                [pltpu.VMEM((clusters,) + tile, BF16)] * (outer // 2),
                pltpu.VMEM((clusters,) + tile, BF16),
                pltpu.VMEM((links,) + tile, BF16),
                pltpu.VMEM((CORES, inner * slots) + tile, BF16),
                pltpu.VMEM((links // 2, patches, patches), BF16),
                pltpu.VMEM(((1 + outer // 2) * links // 2,) + tile, BF16),
                pltpu.VMEM((links,) + tile, BF16),
                pltpu.VMEM((links,) + tile, BF16),
                pltpu.VMEM((links + 1,) + tile, F32),
                pltpu.VMEM((links + 1,) + tile, F32),
                pltpu.VMEM((clusters,) + tile, F32),
                pltpu.VMEM((clusters,) + tile, F32),
                pltpu.VMEM((clusters,) + tile, F32),
                pltpu.VMEM((n, 1, links), jnp.int32),
                pltpu.SMEM((n, 1, links), jnp.int32),
                pltpu.VMEM((links, patches), jnp.int32),
                pltpu.VMEM((4, 1, links), jnp.int32),
                pltpu.SMEM((4, 1, links), jnp.int32),
                pltpu.SemaphoreType.DMA,
                pltpu.SemaphoreType.DMA((7,)),
                pltpu.SemaphoreType.DMA((3,)),
                pltpu.SemaphoreType.DMA((4,)),
                pltpu.SemaphoreType.REGULAR,
                pltpu.SemaphoreType.REGULAR,
                pltpu.SemaphoreType.REGULAR((rounds,)),
                pltpu.SemaphoreType.DMA((2 + outer // 2,)),
                pltpu.SemaphoreType.DMA((3,)),
                pltpu.SemaphoreType.DMA((2 + outer,)),
                pltpu.SemaphoreType.DMA((1 + outer,)),
            ],
            compiler_params=pltpu.CompilerParams(
                collective_id=0, has_side_effects=True, vmem_limit_bytes=EXCHANGE_MIB * 1024 * 1024
            ),
            name="exchange",
        )(
            block_index,
            target_index,
            valid_count,
            source_index,
            radiance,
            patch_area,
            form_factor,
            emission,
            reflectance,
        )

    spec3 = P(("gx", "gy"), None, None)
    spec2 = P(("gx", "gy"), None)
    return jax.shard_map(
        shards,
        mesh=mesh,
        in_specs=(spec3, spec3, spec3, spec2, spec3, spec2, spec2, spec2, spec2),
        out_specs=spec3,
        check_vma=False,
    )
```
